256 devices in a mesh: bank: 32 (over y, z), grp: 8 (over x, core).
Axes of the slice: x: 4, y: 4, z: 8, core: 2. Of those that a mesh axis runs over, the one named last changes fastest.
Arguments:
- users: bfloat16 [32768, 256], P(('bank', 'grp')), may hold values from -32 to 32
- bank: bfloat16 [16384, 256], P('bank'), may hold values from -3 to 3
- positives: int32 [32768], P(('bank', 'grp')), may hold values from 0 to 16383
- cohorts: int32 [32768], P(('bank', 'grp')), may hold values from 0 to 15
Outputs:
- loss: float32 [], replicated
- user_grad: float32 [32768, 256], P(('bank', 'grp'))
- bank_grad: float32 [16384, 256], P(('bank', 'grp'))
The draws below stay inside these ranges and needn't reach their ends.
All inputs are finite; a program needn't handle non-finite values.
Results may differ from the reference program's by a relative error of at most 0.014.
Values may be sent and summed in bfloat16 or wider, within the bound.
No kernel may reach another device: no remote copies, remote signals or barrier semaphores. Data moves between devices by JAX's collectives and lax.ppermute only.
A program may use at most 64 MiB of HBM per device.

```python
import math
import jax
import jax.numpy as jnp
import numpy as np
from jax import lax

E = 256
USER_DEV = 128
ITEM_DEV = 512
NCOH = 16
USERS = 32768
ITEMS = 16384
N_BANK = 32
N_GRP = 8


def bank_values(key):
    base = jax.random.normal(jax.random.fold_in(key, 11), (ITEMS, E), jnp.float32)
    values = 0.25 * jnp.clip(base, -6.0, 6.0)
    return jnp.clip(values, -3.0, 3.0)


def draw_bank(key, part):
    return bank_values(key).astype(jnp.bfloat16)


def draw_users(key, part):
    base = jax.random.normal(jax.random.fold_in(key, 21), (USERS, E), jnp.float32)
    values = 0.75 * jnp.clip(base, -6.0, 6.0)
    return jnp.clip(values, -32.0, 32.0).astype(jnp.bfloat16)


def plant(array, key, smallest, largest):
    spot = [jax.random.randint(jax.random.fold_in(key, axis), (), 0, length) for axis, length in enumerate(array.shape)]
    widest = array.shape.index(max(array.shape))
    next_to = spot[:widest] + [(spot[widest] + 1) % array.shape[widest]] + spot[widest + 1:]
    return array.at[tuple(spot)].set(smallest).at[tuple(next_to)].set(largest)


def cumulative_ranks(number_of, slope):
    loads = [(1 << 20) // math.isqrt(standing ** slope) + 1 for standing in range(1, number_of + 1)]
    scale = 1 + sum(loads) // (1 << 30)
    return np.cumsum(np.array([max(1, weight // scale) for weight in loads]))


def ranked(own_key, dims, number_of, slope):
    grid = cumulative_ranks(number_of, slope)
    ticket = jax.random.randint(jax.random.fold_in(own_key, 1), dims, 0, int(grid[number_of - 1]))
    standing = jnp.searchsorted(jnp.asarray(grid, jnp.int32), ticket, side="right")
    return jax.random.permutation(jax.random.fold_in(own_key, 2), number_of)[standing].astype(jnp.int32)


def setup_inputs(seed: int = 0) -> dict:
    splits = jax.random.split(jax.random.key(seed), 5)
    users = draw_users(jax.random.fold_in(splits[4], 71), 0)
    bank = draw_bank(jax.random.fold_in(splits[4], 71), 0)
    positives = plant(jax.random.randint(splits[2], (USERS,), 0, ITEMS), jax.random.fold_in(splits[2], 1), 0, ITEMS - 1).astype(jnp.int32)
    cohorts = plant(ranked(splits[3], (USERS,), NCOH, 2), jax.random.fold_in(splits[3], 3), 0, NCOH - 1).astype(jnp.int32)
    return dict(users=users, bank=bank, positives=positives, cohorts=cohorts)


def group_pass(users_g, pos_g, coh_g, bank, counts):
    rows = users_g.shape[0]
    block = 512 if rows % 512 == 0 else rows
    count = rows // block
    ub = users_g.reshape(count, block, E)
    pb = pos_g.reshape(count, block)
    cb = coh_g.reshape(count, block)
    cohort_ids = jnp.arange(NCOH, dtype=jnp.int32)
    item_ids = jnp.arange(ITEMS, dtype=jnp.int32)
    bank_blocks = bank.reshape(N_BANK, ITEM_DEV, E).astype(jnp.float32)
    scale = jnp.float32(USERS) / NCOH

    def step(carry, parts):
        upart, ppart, cpart = parts
        logits = jnp.dot(upart, bank.T, preferred_element_type=jnp.float32)
        top = jnp.max(logits, axis=1)
        lse = top + jnp.log(jnp.sum(jnp.exp(logits - top[:, None]), axis=1))
        hot = item_ids[None, :] == ppart[:, None]
        pos_logit = jnp.sum(jnp.where(hot, logits, jnp.float32(0.0)), axis=1)
        own = jnp.sum(jnp.where(cpart[:, None] == cohort_ids[None, :], counts[None, :], jnp.float32(0.0)), axis=1)
        weight = scale / own
        loss_part = jnp.sum(weight * (lse - pos_logit))
        prob = jnp.exp(logits - lse[:, None])
        dlogits = (weight[:, None] * (prob - hot.astype(jnp.float32))).astype(jnp.bfloat16)
        dblocks = dlogits.astype(jnp.float32).reshape(dlogits.shape[0], N_BANK, ITEM_DEV)
        terms = jnp.einsum("ubi,bie->bue", dblocks, bank_blocks, precision=lax.Precision.HIGHEST)
        rounded = lax.optimization_barrier(terms.astype(jnp.bfloat16))
        ugrad = jnp.sum(rounded.astype(jnp.float32), axis=0)
        bacc = carry[0] + jnp.dot(dlogits.astype(jnp.float32).T, upart.astype(jnp.float32), precision=lax.Precision.HIGHEST)
        return (bacc, carry[1] + loss_part), ugrad

    init = (jnp.zeros((ITEMS, E), jnp.float32), jnp.float32(0.0))
    (bacc, loss_sum), ugrads = lax.scan(step, init, (ub, pb, cb))
    return bacc, loss_sum, ugrads.reshape(rows, E)


def reference(users, bank, positives, cohorts):
    cohort_ids = jnp.arange(NCOH, dtype=jnp.int32)
    counts = jnp.sum((cohorts[:, None] == cohort_ids[None, :]).astype(jnp.float32), axis=0)
    ug = users.reshape(N_BANK, N_GRP, USER_DEV, E).transpose(1, 0, 2, 3).reshape(N_GRP, N_BANK * USER_DEV, E)
    pg = positives.reshape(N_BANK, N_GRP, USER_DEV).transpose(1, 0, 2).reshape(N_GRP, N_BANK * USER_DEV)
    cg = cohorts.reshape(N_BANK, N_GRP, USER_DEV).transpose(1, 0, 2).reshape(N_GRP, N_BANK * USER_DEV)

    def outer(carry, parts):
        bacc, loss_sum, ugrads = group_pass(parts[0], parts[1], parts[2], bank, counts)
        rounded = lax.optimization_barrier(bacc.astype(jnp.bfloat16)).astype(jnp.float32)
        return (carry[0] + rounded, carry[1] + loss_sum), ugrads

    init = (jnp.zeros((ITEMS, E), jnp.float32), jnp.float32(0.0))
    (bank_grad, loss_sum), ugrads = lax.scan(outer, init, (ug, pg, cg))
    user_grad = ugrads.reshape(N_GRP, N_BANK, USER_DEV, E).transpose(1, 0, 2, 3).reshape(USERS, E)
    loss = loss_sum / jnp.float32(USERS)
    return loss, user_grad, bank_grad
```

```python
import functools

import jax
import jax.numpy as jnp
from jax import lax
from jax.experimental import pallas as pl
from jax.experimental.pallas import tpu as pltpu
from jax.sharding import Mesh
from jax.sharding import PartitionSpec as P

NCOH = 16
PLANE = ("y", "x")
GROUP = ("c", "y", "x")
COLUMN = ("z", "x", "c")
ALL = ("y", "z", "x", "c")
SHIFT = (0, 4, 1, 5, 7, 3, 2, 6)
F32 = jnp.float32
BF16 = jnp.bfloat16
SHARDS = 4


def exchange(value, axis):
    return lax.all_to_all(value, axis, split_axis=0, concat_axis=0, tiled=True)


def copies(value, n):
    return jnp.broadcast_to(value[None], (n, *value.shape))


def scores(bank, users):
    return lax.dot_general(bank, users, (((1,), (1,)), ((), ())), preferred_element_type=F32)


def lanes(ref, row):
    return jnp.concatenate([ref[s, row : row + 1, :] for s in range(SHARDS)], axis=1)


def forward_kernel(half, users, bank, pos, count, stats_in, stats):
    del half, stats_in
    users = users[...].reshape(SHARDS * users.shape[1], users.shape[2])
    logits = scores(bank[...], users)
    top = jnp.max(logits, axis=0, keepdims=True)
    total = jnp.sum(jnp.exp(logits - top), axis=0, keepdims=True)
    items = lax.broadcasted_iota(jnp.int32, logits.shape, 0)
    own = jnp.sum(jnp.where(items == lanes(pos, 0), logits, F32(0)), axis=0, keepdims=True)
    for s in range(SHARDS):
        cut = slice(s * 128, (s + 1) * 128)
        stats[s, 0:1, :] = top[:, cut]
        stats[s, 1:2, :] = total[:, cut]
        stats[s, 2:3, :] = own[:, cut]
        stats[s, 3:4, :] = count[...]
        stats[s, 4:8, :] = jnp.zeros((4, 128), F32)


def forward(half, users, bank, pos, count, stats):
    shards, rows, width = users.shape
    steps = shards // SHARDS
    at_half = lambda i, h: (h[0] * steps + i, 0, 0)
    whole = lambda i, h: (0, 0)
    return pl.pallas_call(
        forward_kernel,
        grid_spec=pltpu.PrefetchScalarGridSpec(
            num_scalar_prefetch=1,
            grid=(steps,),
            in_specs=[
                pl.BlockSpec((SHARDS, rows, width), lambda i, h: (i, 0, 0)),
                pl.BlockSpec(bank.shape, whole),
                pl.BlockSpec((SHARDS, 1, rows), at_half),
                pl.BlockSpec(count.shape, whole),
                pl.BlockSpec(memory_space=pl.ANY),
            ],
            out_specs=pl.BlockSpec((SHARDS, 8, rows), at_half),
        ),
        out_shape=jax.ShapeDtypeStruct(stats.shape, stats.dtype),
        input_output_aliases={5: 0},
        name="forward",
    )(half, users, bank, pos, count, stats)


def combine_kernel(scale, stats, cohorts, out):
    top = jnp.max(stats[:, 0, :], axis=0, keepdims=True)
    total = jnp.sum(stats[:, 1, :] * jnp.exp(stats[:, 0, :] - top), axis=0, keepdims=True)
    own = jnp.sum(stats[:, 2, :], axis=0, keepdims=True)
    counts = jnp.sum(stats[:, 3, :], axis=0, keepdims=True)
    shape = (NCOH, counts.shape[1])
    row = lax.broadcasted_iota(jnp.int32, shape, 0)
    lane = lax.broadcasted_iota(jnp.int32, shape, 1)
    column = jnp.sum(jnp.where(row == lane, counts, F32(0)), axis=1, keepdims=True)
    mine = jnp.sum(jnp.where(row == cohorts[...], column, F32(0)), axis=0, keepdims=True)
    weight = scale / mine
    lse = top + jnp.log(total)
    loss = jnp.sum(weight * (lse - own), axis=1, keepdims=True)
    rows = lax.broadcasted_iota(jnp.int32, (8, lse.shape[1]), 0)
    tile = jnp.where(rows == 0, lse, jnp.where(rows == 1, weight, jnp.where(rows == 2, loss, F32(0))))
    out[...] = jnp.broadcast_to(tile[None], out.shape)


def backward_kernel(half, users, bank, bank_t, pos, sent, grad_in, user_part, bank_part, acc):
    del half
    step = pl.program_id(0)

    @pl.when(step == 0)
    def _():
        acc[...] = grad_in[...]

    users = users[...].reshape(SHARDS * users.shape[1], users.shape[2])
    logits = scores(bank[...], users)
    items = lax.broadcasted_iota(jnp.int32, logits.shape, 0)
    hot = jnp.where(items == lanes(pos, 0), F32(1), F32(0))
    prob = jnp.exp(logits - lanes(sent, 0))
    dlogits = (lanes(sent, 1) * (prob - hot)).astype(BF16)
    part = jnp.dot(bank_t[...], dlogits, preferred_element_type=F32).astype(BF16)
    for s in range(SHARDS):
        user_part[s] = part[:, s * 128 : (s + 1) * 128]
    acc[...] += jnp.dot(dlogits, users, preferred_element_type=F32)

    @pl.when(step == pl.num_programs(0) - 1)
    def _():
        bank_part[...] = acc[...].astype(bank_part.dtype)


def backward(half, users, bank, bank_t, pos, sent, grad_in, dtype):
    shards, rows, width = users.shape
    steps = shards // SHARDS
    at_half = lambda i, h: (h[0] * steps + i, 0, 0)
    whole = lambda i, h: (0, 0)
    return pl.pallas_call(
        backward_kernel,
        grid_spec=pltpu.PrefetchScalarGridSpec(
            num_scalar_prefetch=1,
            grid=(steps,),
            in_specs=[
                pl.BlockSpec((SHARDS, rows, width), lambda i, h: (i, 0, 0)),
                pl.BlockSpec(bank.shape, whole),
                pl.BlockSpec(bank_t.shape, whole),
                pl.BlockSpec((SHARDS, 1, rows), at_half),
                pl.BlockSpec((SHARDS, 8, rows), at_half),
                pl.BlockSpec(grad_in.shape, whole),
            ],
            out_specs=[
                pl.BlockSpec((SHARDS, width, rows), lambda i, h: (i, 0, 0)),
                pl.BlockSpec(bank.shape, whole),
            ],
            scratch_shapes=[pltpu.VMEM(bank.shape, F32)],
        ),
        out_shape=[
            jax.ShapeDtypeStruct((shards, width, rows), BF16),
            jax.ShapeDtypeStruct(bank.shape, dtype),
        ],
        name="backward",
    )(half, users, bank, bank_t, pos, sent, grad_in)


def finish_kernel(parts, out):
    total = parts[0].astype(F32)
    for k in range(1, parts.shape[0]):
        total = total + parts[k].astype(F32)
    out[...] = total.T


def per_device(users, bank, positives, cohorts):
    rows, width = users.shape
    items_here = bank.shape[0]
    ny, nz, nx, nc = (lax.axis_size(a) for a in ALL)
    plane, group = ny * nx, ny * nx * nc
    total_users = rows * ny * nz * nx * nc
    core = lax.axis_index("c")
    cross = [(k, 1 - k) for k in range(nc)]

    pairs = []
    for z in range(nz):
        for k in range(nx * nc):
            pairs.append((((z + SHIFT[k]) % nz) * nx * nc + k, z * nx * nc + k))
    back = [(b, a) for a, b in pairs]
    column = lax.axis_index("x") * nc + core
    shift = jnp.asarray(SHIFT, jnp.int32)[column]
    block = lax.axis_index("y") * nz + (lax.axis_index("z") + shift) % nz

    near = exchange(copies(users, plane), PLANE)
    pos = exchange(copies(positives[None], group), GROUP)
    item_block = lax.ppermute(bank, COLUMN, pairs)
    ids = jnp.arange(128, dtype=jnp.int32)
    count = jnp.sum((cohorts[:, None] == ids[None, :]).astype(F32), axis=0)
    count = jnp.sum(exchange(copies(count[None], nz), "z"), axis=0)
    pos = pos - block * items_here
    far = lax.ppermute(near, "c", cross)

    here = jnp.reshape(core, (1,)).astype(jnp.int32)
    there = 1 - here
    stats = jnp.zeros((group, 8, rows), F32)
    stats = forward(here, near, item_block, pos, count, stats)
    stats = forward(there, far, item_block, pos, count, stats)
    stats = exchange(stats, GROUP)
    sent = pl.pallas_call(
        functools.partial(combine_kernel, total_users / NCOH),
        out_shape=jax.ShapeDtypeStruct(stats.shape, F32),
        name="combine",
    )(stats, cohorts[None])
    sent = exchange(sent, GROUP)
    loss = jnp.sum(sent[:, 2, :1], axis=0, keepdims=True)
    loss = exchange(jnp.broadcast_to(loss[None], (nz, 1, 128)), "z")
    loss = jnp.sum(loss[:, 0, 0]) / F32(total_users)

    bank_t = item_block.T
    none = jnp.zeros(bank.shape, F32)
    far_part, bank_part = backward(there, far, item_block, bank_t, pos, sent, none, F32)
    far_part = lax.ppermute(far_part, "c", cross)
    near_part, bank_part = backward(here, near, item_block, bank_t, pos, sent, bank_part, BF16)
    user_part = (near_part.astype(F32) + far_part.astype(F32)).astype(BF16)
    user_part = exchange(user_part, PLANE)
    bank_part = lax.ppermute(bank_part, COLUMN, back)
    bank_part = exchange(bank_part.reshape(nx * nc, -1, width), ("x", "c"))
    bank_grad = jnp.sum(bank_part.astype(F32), axis=0)
    user_grad = pl.pallas_call(
        finish_kernel,
        out_shape=jax.ShapeDtypeStruct(users.shape, F32),
        name="finish",
    )(user_part)
    return loss, user_grad, bank_grad


def solution(mesh):
    torus = Mesh(mesh.devices.reshape(4, 8, 4, 2), ALL)
    return jax.shard_map(
        per_device,
        mesh=torus,
        in_specs=(P(ALL, None), P(("y", "z"), None), P(ALL), P(ALL)),
        out_specs=(P(), P(ALL, None), P(ALL, None)),
        check_vma=False,
    )
```

```python
import functools

import jax
import jax.numpy as jnp
from jax import lax
from jax.experimental import pallas as pl
from jax.experimental.pallas import tpu as pltpu
from jax.sharding import Mesh
from jax.sharding import PartitionSpec as P

NCOH = 16
PLANE = ("y", "x")
COLUMN = ("z", "x", "c")
ALL = ("y", "z", "x", "c")
SHIFT = (0, 4, 1, 5, 7, 3, 2, 6)
F32 = jnp.float32
BF16 = jnp.bfloat16
LANES = 128
RADIX = 128
STEP = 4
VMEM = pl.BlockSpec(memory_space=pltpu.VMEM)
SMEM = pl.BlockSpec(memory_space=pltpu.SMEM)


def exchange(value, axis):
    return lax.all_to_all(value, axis, split_axis=0, concat_axis=0, tiled=True)


def copies(value, n):
    return jnp.broadcast_to(value[None], (n, *value.shape))


def summed_along(value, axis):
    n = lax.axis_size(axis)
    total = value
    for by in range(1, n):
        total = total + lax.ppermute(value, axis, [(k, (k + by) % n) for k in range(n)])
    return total


def scores(bank, users):
    return lax.dot_general(bank, users, (((1,), (1,)), ((), ())), preferred_element_type=F32)


def iota(shape, dim):
    return lax.broadcasted_iota(jnp.int32, shape, dim)


def shard_users(packed, at, rows):
    return jnp.concatenate([packed[at + s, :rows, :] for s in range(STEP)], axis=0)


def shard_row(packed, at, row, half):
    cut = slice(half * LANES, (half + 1) * LANES)
    tiles = [packed[at + s, row : row + 8, cut].astype(F32)[0:1] for s in range(STEP)]
    return jnp.concatenate(tiles, axis=1)


def cohort_row(packed, at, rows, half):
    cut = slice(half * LANES, (half + 1) * LANES)
    tiles = [packed[at + s, rows : rows + 8, cut].astype(F32)[1:2] for s in range(STEP)]
    return jnp.concatenate(tiles, axis=1)


def local_positives(packed, at, rows, first):
    high = shard_row(packed, at, rows, 0)
    low = shard_row(packed, at, rows, 1)
    return (high * RADIX + low).astype(jnp.int32) - first


def column_to_row(column):
    shape = (NCOH, LANES)
    spread = jnp.where(iota(shape, 0) == iota(shape, 1), column, F32(0))
    return jnp.sum(spread, axis=0, keepdims=True)


def row_to_column(row):
    shape = (NCOH, LANES)
    spread = jnp.where(iota(shape, 0) == iota(shape, 1), row, F32(0))
    return jnp.sum(spread, axis=1, keepdims=True)


def forward_kernel(rows, first, packed, bank, stats, coh):
    shards = packed.shape[0]
    positive = jnp.zeros((NCOH, 1), F32)
    for at in range(0, shards, STEP):
        logits = scores(bank[...], shard_users(packed, at, rows))
        top = jnp.max(logits, axis=0, keepdims=True)
        total = jnp.sum(jnp.exp(logits - top), axis=0, keepdims=True)
        pos = local_positives(packed, at, rows, first[0])
        own = jnp.sum(jnp.where(iota(logits.shape, 0) == pos, logits, F32(0)), axis=0, keepdims=True)
        lse = top + jnp.log(total)
        mine = cohort_row(packed, at, rows, 0)
        ids = iota((NCOH, mine.shape[1]), 0).astype(F32)
        positive += jnp.sum(jnp.where(ids == mine, own, F32(0)), axis=1, keepdims=True)
        for s in range(STEP):
            cut = slice(s * LANES, (s + 1) * LANES)
            stats[at + s : at + s + 1, :] = lse[:, cut]
            coh[at + s : at + s + 1, :] = mine[:, cut]
    stats[shards : shards + 8, :] = jnp.broadcast_to(column_to_row(positive), (8, LANES))


def forward(packed, bank, first, rows):
    shards = packed.shape[0]
    return pl.pallas_call(
        functools.partial(forward_kernel, rows),
        in_specs=[SMEM, VMEM, VMEM],
        out_specs=[VMEM, VMEM],
        out_shape=[
            jax.ShapeDtypeStruct((shards + 8, LANES), F32),
            jax.ShapeDtypeStruct((shards, LANES), F32),
        ],
        name="forward",
    )(first, packed, bank)


def join_kernel(near, far, other_near, other_far, count, other_count, out):
    shards = near.shape[0] - 8

    def join(a, b):
        top = jnp.maximum(a, b)
        return top + jnp.log(jnp.exp(a - top) + jnp.exp(b - top))

    first = join(near[:shards], other_far[:shards])
    second = join(far[:shards], other_near[:shards])
    positive = near[shards:] + far[shards:] + other_near[shards:] + other_far[shards:]
    counts = count[...] + other_count[...]
    for k in range(out.shape[0]):
        out[k, :shards] = first
        out[k, shards : 2 * shards] = second
        out[k, 2 * shards : 2 * shards + 8] = positive
        out[k, 2 * shards + 8 :] = counts


def settle_kernel(scale, stats, coh_near, coh_far, lse_out, weight_out, loss_out):
    shards = coh_near.shape[0]
    both = 2 * shards
    top = stats[0, :both]
    for k in range(1, stats.shape[0]):
        top = jnp.maximum(top, stats[k, :both])
    total = jnp.exp(stats[0, :both] - top)
    rest = stats[0, both:]
    for k in range(1, stats.shape[0]):
        total += jnp.exp(stats[k, :both] - top)
        rest += stats[k, both:]
    lse = top + jnp.log(total)
    lse_out[...] = lse
    per_cohort = scale / row_to_column(rest[8:9])
    weight_out[...] = jnp.broadcast_to(per_cohort, weight_out.shape)
    weights = jnp.zeros((both, LANES), F32)
    cohorts = jnp.concatenate([coh_near[...], coh_far[...]], axis=0)
    for c in range(NCOH):
        weights = jnp.where(cohorts == F32(c), per_cohort[c : c + 1, :], weights)
    loss = jnp.sum(weights * lse, keepdims=True)
    loss -= jnp.sum(per_cohort * row_to_column(rest[0:1]), keepdims=True)
    loss_out[...] = jnp.broadcast_to(loss, loss_out.shape)


def backward_kernel(rows, half, first, packed, bank, lse, weight, grad_in, user_part, bank_part):
    shards = packed.shape[0]
    total = grad_in[...]
    bank_t = bank[...].T
    for at in range(0, shards, STEP):
        users = shard_users(packed, at, rows)
        logits = scores(bank[...], users)
        pos = local_positives(packed, at, rows, first[0])
        mine = cohort_row(packed, at, rows, 0)
        ids = iota((NCOH, mine.shape[1]), 0).astype(F32)
        weights = jnp.sum(jnp.where(ids == mine, weight[:, 0:1], F32(0)), axis=0, keepdims=True)
        line = half * shards + at
        level = jnp.concatenate([lse[line + s : line + s + 1, :] for s in range(STEP)], axis=1)
        hot = jnp.where(iota(logits.shape, 0) == pos, F32(1), F32(0))
        dlogits = (weights * (jnp.exp(logits - level) - hot)).astype(BF16)
        part = jnp.dot(bank_t, dlogits, preferred_element_type=F32).astype(BF16)
        for s in range(STEP):
            user_part[at + s] = part[:, s * LANES : (s + 1) * LANES]
        total = total + jnp.dot(dlogits, users, preferred_element_type=F32)
    bank_part[...] = total.astype(bank_part.dtype)


def backward(half, packed, bank, first, lse, weight, grad_in, rows, dtype):
    shards, _, width = packed.shape
    return pl.pallas_call(
        functools.partial(backward_kernel, rows, half),
        in_specs=[SMEM] + [VMEM] * 5,
        out_specs=[VMEM, VMEM],
        out_shape=[
            jax.ShapeDtypeStruct((shards, width, rows), BF16),
            jax.ShapeDtypeStruct(bank.shape, dtype),
        ],
        name="backward",
    )(first, packed, bank, lse, weight, grad_in)


def finish_kernel(parts, out):
    total = parts[0].astype(F32)
    for k in range(1, parts.shape[0]):
        total = total + parts[k].astype(F32)
    out[...] = total.T


def per_device(users, bank, positives, cohorts):
    rows, width = users.shape
    ny, nz, nx, nc = (lax.axis_size(a) for a in ALL)
    plane = ny * nx
    total_users = rows * plane * nz * nc
    cross = [(k, 1 - k) for k in range(nc)]

    pairs = []
    for z in range(nz):
        for k in range(nx * nc):
            pairs.append((((z + SHIFT[k]) % nz) * nx * nc + k, z * nx * nc + k))
    back = [(b, a) for a, b in pairs]
    column = lax.axis_index("x") * nc + lax.axis_index("c")
    shift = sum(jnp.where(column == k, SHIFT[k], 0) for k in range(nx * nc))
    block = lax.axis_index("y") * nz + (lax.axis_index("z") + shift) % nz
    first = jnp.reshape(block * bank.shape[0], (1,)).astype(jnp.int32)

    digits = jnp.concatenate([positives // RADIX, positives % RADIX])[None]
    labels = jnp.concatenate([cohorts, jnp.zeros_like(cohorts)])[None]
    extra = jnp.concatenate([digits, labels, jnp.zeros((14, width), jnp.int32)]).astype(BF16)
    packed = jnp.concatenate([users, extra])
    near = exchange(copies(packed, plane), PLANE)
    item_block = lax.ppermute(bank, COLUMN, pairs)
    ids = jnp.arange(LANES, dtype=jnp.int32)
    count = jnp.sum((cohorts[:, None] == ids[None, :]).astype(F32), axis=0)
    count = summed_along(jnp.broadcast_to(count[None], (8, LANES)), "z")
    other_count = lax.ppermute(count, "c", cross)
    far = lax.ppermute(near, "c", cross)

    near_stats, near_coh = forward(near, item_block, first, rows)
    other_near = lax.ppermute(near_stats, "c", cross)
    far_stats, far_coh = forward(far, item_block, first, rows)
    other_far = lax.ppermute(far_stats, "c", cross)
    stats = pl.pallas_call(
        join_kernel,
        in_specs=[VMEM] * 6,
        out_specs=VMEM,
        out_shape=jax.ShapeDtypeStruct((plane, 2 * plane + 16, LANES), F32),
        name="join",
    )(near_stats, far_stats, other_near, other_far, count, other_count)
    stats = exchange(stats, PLANE)
    lse, weight, loss = pl.pallas_call(
        functools.partial(settle_kernel, total_users / NCOH),
        in_specs=[VMEM] * 3,
        out_specs=[VMEM] * 3,
        out_shape=[
            jax.ShapeDtypeStruct((2 * plane, LANES), F32),
            jax.ShapeDtypeStruct((NCOH, LANES), F32),
            jax.ShapeDtypeStruct((8, LANES), F32),
        ],
        name="settle",
    )(stats, near_coh, far_coh)
    loss = summed_along(loss, "z")[0, 0] / F32(total_users)

    none = jnp.zeros(bank.shape, F32)
    far_part, bank_part = backward(1, far, item_block, first, lse, weight, none, rows, F32)
    far_part = lax.ppermute(far_part, "c", cross)
    near_part, bank_part = backward(0, near, item_block, first, lse, weight, bank_part, rows, BF16)
    user_part = (near_part.astype(F32) + far_part.astype(F32)).astype(BF16)
    user_part = exchange(user_part, PLANE)
    bank_part = lax.ppermute(bank_part, COLUMN, back)
    bank_part = exchange(bank_part.reshape(nx * nc, -1, width), ("x", "c"))
    bank_grad = jnp.sum(bank_part.astype(F32), axis=0)
    user_grad = pl.pallas_call(
        finish_kernel,
        in_specs=[VMEM],
        out_specs=VMEM,
        out_shape=jax.ShapeDtypeStruct(users.shape, F32),
        name="finish",
    )(user_part)
    return loss, user_grad, bank_grad


def solution(mesh):
    torus = Mesh(mesh.devices.reshape(4, 8, 4, 2), ALL)
    return jax.shard_map(
        per_device,
        mesh=torus,
        in_specs=(P(ALL, None), P(("y", "z"), None), P(ALL), P(ALL)),
        out_specs=(P(), P(ALL, None), P(ALL, None)),
        check_vma=False,
    )
```

```python
import functools

import jax
import jax.numpy as jnp
from jax import lax
from jax.experimental import pallas as pl
from jax.experimental.pallas import tpu as pltpu
from jax.sharding import Mesh
from jax.sharding import PartitionSpec as P


NCOH = 16
PLANE = ("y", "x")
COLUMN = ("z", "x", "c")
ALL = ("y", "z", "x", "c")
SHIFT = (0, 4, 1, 5, 7, 3, 2, 6)
F32 = jnp.float32
BF16 = jnp.bfloat16
LANES = 128
RADIX = 128
STEP = 4
VMEM = pl.BlockSpec(memory_space=pltpu.VMEM)
SMEM = pl.BlockSpec(memory_space=pltpu.SMEM)


def exchange(value, axis):
    return lax.all_to_all(value, axis, split_axis=0, concat_axis=0, tiled=True)


def copies(value, n):
    return jnp.broadcast_to(value[None], (n, *value.shape))


def scores(bank, users):
    return lax.dot_general(bank, users, (((1,), (1,)), ((), ())), preferred_element_type=F32)


def iota(shape, dim):
    return lax.broadcasted_iota(jnp.int32, shape, dim)


def shard_users(packed, at, rows):
    return jnp.concatenate([packed[at + s, :rows, :] for s in range(STEP)], axis=0)


def shard_row(packed, at, row, half):
    cut = slice(half * LANES, (half + 1) * LANES)
    tiles = [packed[at + s, row : row + 8, cut].astype(F32)[0:1] for s in range(STEP)]
    return jnp.concatenate(tiles, axis=1)


def cohort_row(packed, at, rows, half):
    cut = slice(half * LANES, (half + 1) * LANES)
    tiles = [packed[at + s, rows : rows + 8, cut].astype(F32)[1:2] for s in range(STEP)]
    return jnp.concatenate(tiles, axis=1)


def local_positives(packed, at, rows, first):
    high = shard_row(packed, at, rows, 0)
    low = shard_row(packed, at, rows, 1)
    return (high * RADIX + low).astype(jnp.int32) - first


def column_to_row(column):
    shape = (NCOH, LANES)
    spread = jnp.where(iota(shape, 0) == iota(shape, 1), column, F32(0))
    return jnp.sum(spread, axis=0, keepdims=True)


def row_to_column(row):
    shape = (NCOH, LANES)
    spread = jnp.where(iota(shape, 0) == iota(shape, 1), row, F32(0))
    return jnp.sum(spread, axis=1, keepdims=True)


def forward_kernel(rows, first, packed, bank, stats, coh):
    shards = packed.shape[0]
    positive = jnp.zeros((NCOH, 1), F32)
    count = jnp.zeros((NCOH, 1), F32)
    for at in range(0, shards, STEP):
        logits = scores(bank[...], shard_users(packed, at, rows))
        top = jnp.max(logits, axis=0, keepdims=True)
        total = jnp.sum(jnp.exp(logits - top), axis=0, keepdims=True)
        pos = local_positives(packed, at, rows, first[0])
        own = jnp.sum(jnp.where(iota(logits.shape, 0) == pos, logits, F32(0)), axis=0, keepdims=True)
        lse = top + jnp.log(total)
        mine = cohort_row(packed, at, rows, 0)
        ids = iota((NCOH, mine.shape[1]), 0).astype(F32)
        positive += jnp.sum(jnp.where(ids == mine, own, F32(0)), axis=1, keepdims=True)
        count += jnp.sum(jnp.where(ids == mine, F32(1), F32(0)), axis=1, keepdims=True)
        for s in range(STEP):
            cut = slice(s * LANES, (s + 1) * LANES)
            stats[at + s : at + s + 1, :] = lse[:, cut]
            coh[at + s : at + s + 1, :] = mine[:, cut]
    extra = jnp.where(iota((8, LANES), 0) == 0, column_to_row(positive), column_to_row(count))
    stats[shards : shards + 8, :] = extra


def forward(packed, bank, first, rows):
    shards = packed.shape[0]
    return pl.pallas_call(
        functools.partial(forward_kernel, rows),
        in_specs=[SMEM, VMEM, VMEM],
        out_specs=[VMEM, VMEM],
        out_shape=[
            jax.ShapeDtypeStruct((shards + 8, LANES), F32),
            jax.ShapeDtypeStruct((shards, LANES), F32),
        ],
        name="forward",
    )(first, packed, bank)


def join_kernel(near, far, other_near, other_far, count, out):
    shards = near.shape[0] - 8

    def join(a, b):
        top = jnp.maximum(a, b)
        return top + jnp.log(jnp.exp(a - top) + jnp.exp(b - top))

    first = join(near[:shards], other_far[:shards])
    second = join(far[:shards], other_near[:shards])
    positive = near[shards:] + far[shards:] + other_near[shards:] + other_far[shards:]
    extra = jnp.where(iota(positive.shape, 0) == 0, positive, count[...])
    for k in range(out.shape[0]):
        out[k, :shards] = first
        out[k, shards : 2 * shards] = second
        out[k, 2 * shards :] = extra


def settle_kernel(scale, repeats, stats, coh_near, coh_far, lse_out, weight_out, loss_out):
    shards = coh_near.shape[0]
    both = 2 * shards
    top = stats[0, :both]
    for k in range(1, stats.shape[0]):
        top = jnp.maximum(top, stats[k, :both])
    total = jnp.exp(stats[0, :both] - top)
    rest = stats[0, both:]
    for k in range(1, stats.shape[0]):
        total += jnp.exp(stats[k, :both] - top)
        rest += stats[k, both:]
    lse = top + jnp.log(total)
    lse_out[...] = lse
    per_cohort = scale * repeats / row_to_column(rest[1:2])
    weight_out[...] = jnp.broadcast_to(per_cohort, weight_out.shape)
    weights = jnp.zeros((both, LANES), F32)
    cohorts = jnp.concatenate([coh_near[...], coh_far[...]], axis=0)
    for c in range(NCOH):
        weights = jnp.where(cohorts == F32(c), per_cohort[c : c + 1, :], weights)
    loss = jnp.sum(weights * lse, keepdims=True)
    loss -= jnp.sum(per_cohort * row_to_column(rest[0:1]), keepdims=True)
    loss_out[...] = jnp.broadcast_to(loss, loss_out.shape)


def backward_core(rows, half, first, packed, bank, lse, weight, user_part, total):
    shards = packed.shape[0]
    bank_t = bank[...].T
    for at in range(0, shards, STEP):
        users = shard_users(packed, at, rows)
        logits = scores(bank[...], users)
        pos = local_positives(packed, at, rows, first[0])
        mine = cohort_row(packed, at, rows, 0)
        ids = iota((NCOH, mine.shape[1]), 0).astype(F32)
        weights = jnp.sum(jnp.where(ids == mine, weight[:, 0:1], F32(0)), axis=0, keepdims=True)
        line = half * shards + at
        level = jnp.concatenate([lse[line + s : line + s + 1, :] for s in range(STEP)], axis=1)
        hot = jnp.where(iota(logits.shape, 0) == pos, F32(1), F32(0))
        dlogits = (weights * (jnp.exp(logits - level) - hot)).astype(BF16)
        part = jnp.dot(bank_t, dlogits, preferred_element_type=F32).astype(BF16)
        for s in range(STEP):
            user_part[at + s] = part[:, s * LANES : (s + 1) * LANES]
        grad = jnp.dot(dlogits, users, preferred_element_type=F32)
        total = grad if total is None else total + grad
    return total


def backward_far_kernel(rows, first, packed, bank, lse, weight, user_part, bank_part):
    bank_part[...] = backward_core(rows, 1, first, packed, bank, lse, weight, user_part, None)


def digits_of(value):
    high = value.astype(BF16)
    rest = value - high.astype(F32)
    mid = rest.astype(BF16)
    low = (rest - mid.astype(F32)).astype(BF16)
    row = iota(value.shape, 0)
    zero = F32(0)
    tile = jnp.where(row == 0, high.astype(F32), zero)
    tile = jnp.where(row == 1, mid.astype(F32), tile)
    return jnp.where(row == 2, low.astype(F32), tile).astype(BF16)


def backward_near_kernel(rows, first, packed, bank, lse, weight, far_part, loss, user_part, *rest):
    pieces, acc = rest[:-1], rest[-1]
    acc[...] = backward_core(rows, 0, first, packed, bank, lse, weight, user_part, far_part[...])
    height = acc.shape[0] // len(pieces)
    tile = digits_of(loss[...])
    for k, piece in enumerate(pieces):
        at = pl.multiple_of(((first[1] + k) % len(pieces)) * height, height)
        piece[:height, :] = acc[pl.ds(at, height), :].astype(BF16)
        piece[height:, :LANES] = tile
        piece[height:, LANES:] = tile


def backward_far(packed, bank, first, lse, weight, rows):
    shards, _, width = packed.shape
    return pl.pallas_call(
        functools.partial(backward_far_kernel, rows),
        in_specs=[SMEM] + [VMEM] * 4,
        out_specs=[VMEM, VMEM],
        out_shape=[
            jax.ShapeDtypeStruct((shards, width, rows), BF16),
            jax.ShapeDtypeStruct(bank.shape, F32),
        ],
        name="backward_far",
    )(first, packed, bank, lse, weight)


def backward_near(packed, bank, first, lse, weight, far_part, loss, rows, pieces):
    shards, _, width = packed.shape
    piece = jax.ShapeDtypeStruct((bank.shape[0] // pieces + 8, width), BF16)
    return pl.pallas_call(
        functools.partial(backward_near_kernel, rows),
        in_specs=[SMEM] + [VMEM] * 6,
        out_specs=[VMEM] * (1 + pieces),
        out_shape=[jax.ShapeDtypeStruct((shards, width, rows), BF16)] + [piece] * pieces,
        scratch_shapes=[pltpu.VMEM(bank.shape, F32)],
        name="backward_near",
    )(first, packed, bank, lse, weight, far_part, loss)


def finish_kernel(parts, out):
    total = parts[0].astype(F32)
    for k in range(1, parts.shape[0]):
        total = total + parts[k].astype(F32)
    out[...] = total.T


def gather_kernel(share, *refs):
    pieces, (grad, loss) = refs[:-2], refs[-2:]
    height = grad.shape[0]
    total = pieces[0][...].astype(F32)
    for piece in pieces[1:]:
        total = total + piece[...].astype(F32)
    grad[...] = total[:height]
    tail = total[height:]
    loss[...] = (jnp.sum(tail, axis=0, keepdims=True) * share)[:, :LANES]


def step(users, bank, positives, cohorts):
    rows, width = users.shape
    ny, nz, nx, nc = (lax.axis_size(a) for a in ALL)
    plane = ny * nx
    total_users = rows * plane * nz * nc
    cross = [(k, 1 - k) for k in range(nc)]

    cols = nx * nc
    fetch = [
        (((z + SHIFT[k]) % nz) * cols + k, z * cols + k) for z in range(nz) for k in range(cols)
    ]
    column = lax.axis_index("x") * nc + lax.axis_index("c")
    shift = sum(jnp.where(column == k, SHIFT[k], 0) for k in range(cols))
    block = lax.axis_index("y") * nz + (lax.axis_index("z") + shift) % nz
    first = jnp.stack([block * bank.shape[0], column]).astype(jnp.int32)

    turn = lambda y, x: (y * nx + x) % nz
    counts_from = [
        ((y * nz + (z + turn(y, x)) % nz) * nx + x, (y * nz + z) * nx + x)
        for y in range(ny)
        for z in range(nz)
        for x in range(nx)
    ]
    repeats = plane // nz

    item_block = lax.ppermute(bank, COLUMN, fetch)
    digits = jnp.concatenate([positives // RADIX, positives % RADIX])[None]
    labels = jnp.concatenate([cohorts, jnp.zeros_like(cohorts)])[None]
    extra = jnp.concatenate([digits, labels, jnp.zeros((14, width), jnp.int32)]).astype(BF16)
    packed = jnp.concatenate([users, extra])
    near = exchange(copies(packed, plane), PLANE)
    far = lax.ppermute(near, "c", cross)

    near_stats, near_coh = forward(near, item_block, first, rows)
    count = lax.ppermute(near_stats[plane:], ("y", "z", "x"), counts_from)
    other_near = lax.ppermute(near_stats, "c", cross)
    far_stats, far_coh = forward(far, item_block, first, rows)
    other_far = lax.ppermute(far_stats, "c", cross)
    count = count + lax.ppermute(count, "c", cross)
    stats = pl.pallas_call(
        join_kernel,
        in_specs=[VMEM] * 5,
        out_specs=VMEM,
        out_shape=jax.ShapeDtypeStruct((plane, 2 * plane + 8, LANES), F32),
        name="join",
    )(near_stats, far_stats, other_near, other_far, count)
    stats = exchange(stats, PLANE)
    lse, weight, loss = pl.pallas_call(
        functools.partial(settle_kernel, total_users / NCOH, repeats),
        in_specs=[VMEM] * 3,
        out_specs=[VMEM] * 3,
        out_shape=[
            jax.ShapeDtypeStruct((2 * plane, LANES), F32),
            jax.ShapeDtypeStruct((NCOH, LANES), F32),
            jax.ShapeDtypeStruct((8, LANES), F32),
        ],
        name="settle",
    )(stats, near_coh, far_coh)

    far_part, bank_part = backward_far(far, item_block, first, lse, weight, rows)
    far_part = lax.ppermute(far_part, "c", cross)
    near_part, *pieces = backward_near(near, item_block, first, lse, weight, bank_part, loss, rows, cols)
    user_part = (near_part.astype(F32) + far_part.astype(F32)).astype(BF16)
    user_part = exchange(user_part, PLANE)
    arrived = []
    for turned, piece in enumerate(pieces):
        ways = [
            (z * cols + k, ((z + SHIFT[k]) % nz) * cols + (k + turned) % cols)
            for z in range(nz)
            for k in range(cols)
        ]
        arrived.append(lax.ppermute(piece, COLUMN, ways))
    bank_grad, loss = pl.pallas_call(
        functools.partial(gather_kernel, 1.0 / total_users),
        in_specs=[VMEM] * cols,
        out_specs=[VMEM] * 2,
        out_shape=[
            jax.ShapeDtypeStruct((bank.shape[0] // cols, width), F32),
            jax.ShapeDtypeStruct((1, LANES), F32),
        ],
        name="gather",
    )(*arrived)
    user_grad = pl.pallas_call(
        finish_kernel,
        in_specs=[VMEM],
        out_specs=VMEM,
        out_shape=jax.ShapeDtypeStruct(users.shape, F32),
        name="finish",
    )(user_part)
    return loss[0, 0], user_grad, bank_grad


def solution(mesh):
    torus = Mesh(mesh.devices.reshape(4, 8, 4, 2), ALL)
    return jax.shard_map(
        step,
        mesh=torus,
        in_specs=(P(ALL, None), P(("y", "z"), None), P(ALL), P(ALL)),
        out_specs=(P(), P(ALL, None), P(ALL, None)),
        check_vma=False,
    )
```

```python
import functools

import jax
import jax.numpy as jnp
from jax import lax
from jax.experimental import pallas as pl
from jax.experimental.pallas import tpu as pltpu
from jax.sharding import Mesh
from jax.sharding import PartitionSpec as P


NCOH = 16
PLANE = ("y", "x")
COLUMN = ("z", "x", "c")
ALL = ("y", "z", "x", "c")
SHIFT = (0, 4, 1, 5, 7, 3, 2, 6)
F32 = jnp.float32
BF16 = jnp.bfloat16
LANES = 128
RADIX = 128
STEP = 4
VMEM = pl.BlockSpec(memory_space=pltpu.VMEM)


def call(kernel, out_shape, *operands, scratch=()):
    return pl.pallas_call(
        kernel,
        in_specs=[VMEM] * len(operands),
        out_specs=jax.tree.map(lambda _: VMEM, out_shape),
        out_shape=out_shape,
        scratch_shapes=list(scratch),
        compiler_params=pltpu.CompilerParams(vmem_limit_bytes=24 << 20),
    )(*operands)


def f32(*shape):
    return jax.ShapeDtypeStruct(shape, F32)


def bf16(*shape):
    return jax.ShapeDtypeStruct(shape, BF16)


def first_item(items):
    column = lax.axis_index("x") * lax.axis_size("c") + lax.axis_index("c")
    shift = sum(jnp.where(column == k, by, 0) for k, by in enumerate(SHIFT))
    nz = lax.axis_size("z")
    return (lax.axis_index("y") * nz + (lax.axis_index("z") + shift) % nz) * items


def exchange(value, axis):
    return lax.all_to_all(value, axis, split_axis=0, concat_axis=0, tiled=True)


def copies(value, n):
    return jnp.broadcast_to(value[None], (n, *value.shape))


def scores(bank, users):
    return lax.dot_general(bank, users, (((1,), (1,)), ((), ())), preferred_element_type=F32)


def iota(shape, dim):
    return lax.broadcasted_iota(jnp.int32, shape, dim)


def shard_users(packed, at, rows):
    return jnp.concatenate([packed[at + s, :rows, :] for s in range(STEP)], axis=0)


def shard_row(packed, at, row, half):
    cut = slice(half * LANES, (half + 1) * LANES)
    tiles = [packed[at + s, row : row + 8, cut].astype(F32)[0:1] for s in range(STEP)]
    return jnp.concatenate(tiles, axis=1)


def cohort_row(packed, at, rows, half):
    cut = slice(half * LANES, (half + 1) * LANES)
    tiles = [packed[at + s, rows : rows + 8, cut].astype(F32)[1:2] for s in range(STEP)]
    return jnp.concatenate(tiles, axis=1)


def local_positives(packed, at, rows, first):
    high = shard_row(packed, at, rows, 0)
    low = shard_row(packed, at, rows, 1)
    return (high * RADIX + low).astype(jnp.int32) - first


def column_to_row(column):
    shape = (NCOH, LANES)
    spread = jnp.where(iota(shape, 0) == iota(shape, 1), column, F32(0))
    return jnp.sum(spread, axis=0, keepdims=True)


def row_to_column(row):
    shape = (NCOH, LANES)
    spread = jnp.where(iota(shape, 0) == iota(shape, 1), row, F32(0))
    return jnp.sum(spread, axis=1, keepdims=True)


def forward_kernel(rows, packed, bank, stats, coh, counts):
    shards = packed.shape[0]
    first = first_item(bank.shape[0])
    positive = jnp.zeros((NCOH, 1), F32)
    count = jnp.zeros((NCOH, 1), F32)
    for at in range(0, shards, STEP):
        logits = scores(bank[...], shard_users(packed, at, rows))
        top = jnp.max(logits, axis=0, keepdims=True)
        total = jnp.sum(jnp.exp(logits - top), axis=0, keepdims=True)
        pos = local_positives(packed, at, rows, first)
        own = jnp.sum(jnp.where(iota(logits.shape, 0) == pos, logits, F32(0)), axis=0, keepdims=True)
        lse = top + jnp.log(total)
        mine = cohort_row(packed, at, rows, 0)
        ids = iota((NCOH, mine.shape[1]), 0).astype(F32)
        positive += jnp.sum(jnp.where(ids == mine, own, F32(0)), axis=1, keepdims=True)
        count += jnp.sum(jnp.where(ids == mine, F32(1), F32(0)), axis=1, keepdims=True)
        for s in range(STEP):
            cut = slice(s * LANES, (s + 1) * LANES)
            stats[at + s : at + s + 1, :] = lse[:, cut]
            coh[at + s : at + s + 1, :] = mine[:, cut]
    stats[shards:, :] = jnp.broadcast_to(column_to_row(positive), (8, LANES))
    counts[...] = jnp.broadcast_to(column_to_row(count), (8, LANES))


def forward(packed, bank, rows):
    shards = packed.shape[0]
    shapes = (f32(shards + 8, LANES), f32(shards, LANES), f32(8, LANES))
    return call(functools.partial(forward_kernel, rows), shapes, packed, bank)


def join_kernel(near, far, other_near, other_far, count, other_count, out):
    shards = near.shape[0] - 8

    def join(a, b):
        top = jnp.maximum(a, b)
        return top + jnp.log(jnp.exp(a - top) + jnp.exp(b - top))

    first = join(near[:shards], other_far[:shards])
    second = join(far[:shards], other_near[:shards])
    positive = near[shards:] + far[shards:] + other_near[shards:] + other_far[shards:]
    extra = jnp.where(iota(positive.shape, 0) == 0, positive, count[...] + other_count[...])
    for k in range(out.shape[0]):
        out[k, :shards] = first
        out[k, shards : 2 * shards] = second
        out[k, 2 * shards :] = extra


def settle(scale, repeats, stats, coh_near, coh_far, lse_out, weight_out, loss_out):
    shards = coh_near.shape[0]
    both = 2 * shards
    top = stats[0, :both]
    for k in range(1, stats.shape[0]):
        top = jnp.maximum(top, stats[k, :both])
    total = jnp.exp(stats[0, :both] - top)
    rest = stats[0, both:]
    for k in range(1, stats.shape[0]):
        total += jnp.exp(stats[k, :both] - top)
        rest += stats[k, both:]
    lse = top + jnp.log(total)
    lse_out[...] = lse
    per_cohort = scale * repeats / row_to_column(rest[1:2])
    weight_out[...] = jnp.broadcast_to(per_cohort, weight_out.shape)
    weights = jnp.zeros((both, LANES), F32)
    cohorts = jnp.concatenate([coh_near[...], coh_far[...]], axis=0)
    for c in range(NCOH):
        weights = jnp.where(cohorts == F32(c), per_cohort[c : c + 1, :], weights)
    loss = jnp.sum(weights * lse, keepdims=True)
    loss -= jnp.sum(per_cohort * row_to_column(rest[0:1]), keepdims=True)
    loss_out[...] = jnp.broadcast_to(loss, loss_out.shape)


def backward_core(rows, half, packed, bank, lse, weight, user_part, total):
    shards = packed.shape[0]
    bank_t = bank[...].T
    first = first_item(bank.shape[0])
    for at in range(0, shards, STEP):
        users = shard_users(packed, at, rows)
        logits = scores(bank[...], users)
        pos = local_positives(packed, at, rows, first)
        mine = cohort_row(packed, at, rows, 0)
        ids = iota((NCOH, mine.shape[1]), 0).astype(F32)
        weights = jnp.sum(jnp.where(ids == mine, weight[:, 0:1], F32(0)), axis=0, keepdims=True)
        line = half * shards + at
        level = jnp.concatenate([lse[line + s : line + s + 1, :] for s in range(STEP)], axis=1)
        hot = jnp.where(iota(logits.shape, 0) == pos, F32(1), F32(0))
        dlogits = (weights * (jnp.exp(logits - level) - hot)).astype(BF16)
        part = jnp.dot(bank_t, dlogits, preferred_element_type=F32).astype(BF16)
        for s in range(STEP):
            user_part[at + s] = part[:, s * LANES : (s + 1) * LANES]
        grad = jnp.dot(dlogits, users, preferred_element_type=F32)
        total = grad if total is None else total + grad
    return total


def backward_far_kernel(rows, scale, repeats, packed, bank, stats, coh_near, coh_far, *outs):
    user_part, bank_part, lse, weight, loss = outs
    settle(scale, repeats, stats, coh_near, coh_far, lse, weight, loss)
    bank_part[...] = backward_core(rows, 1, packed, bank, lse, weight, user_part, None)


def digits_of(value):
    high = value.astype(BF16)
    rest = value - high.astype(F32)
    mid = rest.astype(BF16)
    low = (rest - mid.astype(F32)).astype(BF16)
    row = iota(value.shape, 0)
    zero = F32(0)
    tile = jnp.where(row == 0, high.astype(F32), zero)
    tile = jnp.where(row == 1, mid.astype(F32), tile)
    return jnp.where(row == 2, low.astype(F32), tile).astype(BF16)


def read_digits(tile):
    return jnp.sum(tile.astype(F32), axis=0, keepdims=True)[:, :LANES]


def write_digits(out, at, value):
    tile = digits_of(jnp.broadcast_to(value, (8, LANES)))
    out[at : at + 8, :LANES] = tile
    out[at : at + 8, LANES:] = tile


def backward_near_kernel(rows, packed, bank, lse, weight, far_part, loss, user_part, out, acc):
    acc[...] = backward_core(rows, 0, packed, bank, lse, weight, user_part, far_part[...])
    nx, nc = lax.axis_size("x"), lax.axis_size("c")
    height = acc.shape[0] // (nx * nc)
    core = lax.axis_index("c")
    for side, owner in enumerate((1 - core, core)):
        for r in range(nx):
            piece = (lax.axis_index("x") + r) % nx * nc + owner
            at = pl.multiple_of(piece * height, height)
            to = side * (nx * height + 8) + r * height
            out[to : to + height, :] = acc[pl.ds(at, height), :].astype(BF16)
    write_digits(out, nx * height, loss[...])


def halve_kernel(mine, theirs, *pieces):
    below = theirs.shape[0]
    height = (below - 8) // len(pieces)
    loss = read_digits(mine[below - 8 : below, :]) + read_digits(theirs[below - 8 :, :])
    for r, piece in enumerate(pieces):
        cut = slice(below + r * height, below + (r + 1) * height)
        own = mine[cut, :].astype(F32) + theirs[r * height : (r + 1) * height, :].astype(F32)
        piece[:height, :] = own.astype(BF16)
        write_digits(piece, height, loss)


def gather_kernel(share, *refs):
    pieces, (grad, loss) = refs[:-2], refs[-2:]
    height = grad.shape[0]
    total = pieces[0][...].astype(F32)
    for piece in pieces[1:]:
        total = total + piece[...].astype(F32)
    grad[...] = total[:height]
    loss[...] = jnp.sum(total[height:], axis=0, keepdims=True)[:, :LANES] * share


def step(users, bank, positives, cohorts):
    rows, width = users.shape
    ny, nz, nx, nc = (lax.axis_size(a) for a in ALL)
    plane = ny * nx
    total_users = rows * plane * nz * nc
    cross = [(k, 1 - k) for k in range(nc)]

    cols = nx * nc
    fetch = [
        (((z + SHIFT[k]) % nz) * cols + k, z * cols + k) for z in range(nz) for k in range(cols)
    ]
    turn = lambda y, x: (y * nx + x) % nz
    counts_from = [
        ((y * nz + (z + turn(y, x)) % nz) * nx + x, (y * nz + z) * nx + x)
        for y in range(ny)
        for z in range(nz)
        for x in range(nx)
    ]
    repeats = plane // nz

    item_block = lax.ppermute(bank, COLUMN, fetch)
    digits = jnp.concatenate([positives // RADIX, positives % RADIX])[None]
    labels = jnp.concatenate([cohorts, jnp.zeros_like(cohorts)])[None]
    extra = jnp.concatenate([digits, labels, jnp.zeros((6, width), jnp.int32)]).astype(BF16)
    packed = jnp.concatenate([users, extra])
    near = exchange(copies(packed, plane), PLANE)
    far = lax.ppermute(near, "c", cross)

    near_stats, near_coh, count = forward(near, item_block, rows)
    count = lax.ppermute(count, ("y", "z", "x"), counts_from)
    other_near = lax.ppermute(near_stats, "c", cross)
    far_stats, far_coh, _ = forward(far, item_block, rows)
    other_count = lax.ppermute(count, "c", cross)
    other_far = lax.ppermute(far_stats, "c", cross)
    stats = call(
        join_kernel,
        f32(plane, 2 * plane + 8, LANES),
        *(near_stats, far_stats, other_near, other_far, count, other_count),
    )
    stats = exchange(stats, PLANE)

    far_part, bank_part, lse, weight, loss = call(
        functools.partial(backward_far_kernel, rows, total_users / NCOH, repeats),
        (
            bf16(plane, width, rows),
            f32(*bank.shape),
            f32(2 * plane, LANES),
            f32(NCOH, LANES),
            f32(8, LANES),
        ),
        *(far, item_block, stats, near_coh, far_coh),
    )
    far_part = lax.ppermute(far_part, "c", cross)
    near_part, bank_part = call(
        functools.partial(backward_near_kernel, rows),
        (bf16(plane, width, rows), bf16(bank.shape[0] + 8, width)),
        *(near, item_block, lse, weight, bank_part, loss),
        scratch=[pltpu.VMEM(bank.shape, F32)],
    )
    bank_part = lax.ppermute(bank_part, COLUMN, [(b, a) for a, b in fetch])
    user_part = near_part + far_part
    user_part = exchange(user_part, PLANE)
    half = bank.shape[0] // nc
    height = half // nx
    theirs = lax.ppermute(bank_part[: half + 8], "c", cross)
    pieces = call(halve_kernel, (bf16(height + 8, width),) * nx, bank_part, theirs)
    arrived = [pieces[0]]
    for r in range(1, nx):
        arrived.append(lax.ppermute(pieces[r], "x", [(k, (k + r) % nx) for k in range(nx)]))
    bank_grad, loss = call(
        functools.partial(gather_kernel, 1.0 / total_users),
        (f32(height, width), f32(1, LANES)),
        *arrived,
    )
    user_grad = jnp.sum(user_part.astype(F32), axis=0).T
    return loss[0, 0], user_grad, bank_grad


def solution(mesh):
    torus = Mesh(mesh.devices.reshape(4, 8, 4, 2), ALL)
    return jax.shard_map(
        step,
        mesh=torus,
        in_specs=(P(ALL, None), P(("y", "z"), None), P(ALL), P(ALL)),
        out_specs=(P(), P(ALL, None), P(ALL, None)),
        check_vma=False,
    )
```

```python
import functools

import jax
import jax.numpy as jnp
from jax import lax
from jax.experimental import pallas as pl
from jax.experimental.pallas import tpu as pltpu
from jax.sharding import Mesh
from jax.sharding import PartitionSpec as P


NCOH = 16
PLANE = ("y", "x")
COLUMN = ("z", "x", "c")
ALL = ("y", "z", "x", "c")
SHIFT = (0, 4, 1, 5, 7, 3, 2, 6)
F32 = jnp.float32
BF16 = jnp.bfloat16
LANES = 128
RADIX = 128
STEP = 4
VMEM = pl.BlockSpec(memory_space=pltpu.VMEM)


def call(kernel, out_shape, *operands, scratch=(), limit=24 << 20):
    return pl.pallas_call(
        kernel,
        in_specs=[VMEM] * len(operands),
        out_specs=jax.tree.map(lambda _: VMEM, out_shape),
        out_shape=out_shape,
        scratch_shapes=list(scratch),
        compiler_params=pltpu.CompilerParams(vmem_limit_bytes=limit),
    )(*operands)


def f32(*shape):
    return jax.ShapeDtypeStruct(shape, F32)


def bf16(*shape):
    return jax.ShapeDtypeStruct(shape, BF16)


def first_item(items):
    column = lax.axis_index("x") * lax.axis_size("c") + lax.axis_index("c")
    shift = sum(jnp.where(column == k, by, 0) for k, by in enumerate(SHIFT))
    nz = lax.axis_size("z")
    return (lax.axis_index("y") * nz + (lax.axis_index("z") + shift) % nz) * items


def exchange(value, axis):
    return lax.all_to_all(value, axis, split_axis=0, concat_axis=0, tiled=True)


def scores(bank, users):
    return lax.dot_general(bank, users, (((1,), (1,)), ((), ())), preferred_element_type=F32)


def iota(shape, dim):
    return lax.broadcasted_iota(jnp.int32, shape, dim)


def shard_users(packed, at, rows):
    return jnp.concatenate([packed[at + s, :rows, :] for s in range(STEP)], axis=0)


def shard_row(packed, at, row, half):
    cut = slice(half * LANES, (half + 1) * LANES)
    tiles = [packed[at + s, row : row + 8, cut].astype(F32)[0:1] for s in range(STEP)]
    return jnp.concatenate(tiles, axis=1)


def cohort_row(packed, at, rows, half):
    cut = slice(half * LANES, (half + 1) * LANES)
    tiles = [packed[at + s, rows : rows + 8, cut].astype(F32)[1:2] for s in range(STEP)]
    return jnp.concatenate(tiles, axis=1)


def local_positives(packed, at, rows, first):
    high = shard_row(packed, at, rows, 0)
    low = shard_row(packed, at, rows, 1)
    return (high * RADIX + low).astype(jnp.int32) - first


def column_to_row(column):
    shape = (NCOH, LANES)
    spread = jnp.where(iota(shape, 0) == iota(shape, 1), column, F32(0))
    return jnp.sum(spread, axis=0, keepdims=True)


def row_to_column(row):
    shape = (NCOH, LANES)
    spread = jnp.where(iota(shape, 0) == iota(shape, 1), row, F32(0))
    return jnp.sum(spread, axis=1, keepdims=True)


def pack_kernel(users, positives, cohorts, out, count):
    rows, _ = users.shape
    pos = positives[...]
    high = (pos // RADIX).astype(F32)
    low = (pos % RADIX).astype(F32)
    mine = cohorts[...].astype(F32)
    row = iota((8, LANES), 0)
    left = jnp.where(row == 0, high, jnp.where(row == 1, mine, F32(0))).astype(BF16)
    right = jnp.where(row == 0, low, F32(0)).astype(BF16)
    for k in range(out.shape[0]):
        out[k, :rows, :] = users[...]
        out[k, rows:, :LANES] = left
        out[k, rows:, LANES:] = right
    ids = iota((NCOH, LANES), 0).astype(F32)
    column = jnp.sum(jnp.where(ids == mine, F32(1), F32(0)), axis=1, keepdims=True)
    count[...] = jnp.broadcast_to(column_to_row(column), (8, LANES))


def forward_kernel(rows, packed, bank, stats, coh):
    shards = packed.shape[0]
    first = first_item(bank.shape[0])
    positive = jnp.zeros((NCOH, 1), F32)
    for at in range(0, shards, STEP):
        logits = scores(bank[...], shard_users(packed, at, rows))
        top = jnp.max(logits, axis=0, keepdims=True)
        total = jnp.sum(jnp.exp(logits - top), axis=0, keepdims=True)
        pos = local_positives(packed, at, rows, first)
        own = jnp.sum(jnp.where(iota(logits.shape, 0) == pos, logits, F32(0)), axis=0, keepdims=True)
        lse = top + jnp.log(total)
        mine = cohort_row(packed, at, rows, 0)
        ids = iota((NCOH, mine.shape[1]), 0).astype(F32)
        positive += jnp.sum(jnp.where(ids == mine, own, F32(0)), axis=1, keepdims=True)
        for s in range(STEP):
            cut = slice(s * LANES, (s + 1) * LANES)
            stats[at + s : at + s + 1, :] = lse[:, cut]
            coh[at + s : at + s + 1, :] = mine[:, cut]
    stats[shards:, :] = jnp.broadcast_to(column_to_row(positive), (8, LANES))


def forward(packed, bank, rows):
    shards = packed.shape[0]
    shapes = (f32(shards + 8, LANES), f32(shards, LANES))
    return call(functools.partial(forward_kernel, rows), shapes, packed, bank)


def join_kernel(near, far, other_near, other_far, count, out):
    shards = near.shape[0] - 8

    def join(a, b):
        top = jnp.maximum(a, b)
        return top + jnp.log(jnp.exp(a - top) + jnp.exp(b - top))

    first = join(near[:shards], other_far[:shards])
    second = join(far[:shards], other_near[:shards])
    positive = near[shards:] + far[shards:] + other_near[shards:] + other_far[shards:]
    extra = jnp.where(iota(positive.shape, 0) == 0, positive, count[...])
    for k in range(out.shape[0]):
        out[k, :shards] = first
        out[k, shards : 2 * shards] = second
        out[k, 2 * shards :] = extra


def settle(scale, stats, coh_near, coh_far, lse_out, weight_out, loss_out):
    shards = coh_near.shape[0]
    both = 2 * shards
    top = stats[0, :both]
    for k in range(1, stats.shape[0]):
        top = jnp.maximum(top, stats[k, :both])
    total = jnp.exp(stats[0, :both] - top)
    rest = stats[0, both:]
    for k in range(1, stats.shape[0]):
        total += jnp.exp(stats[k, :both] - top)
        rest += stats[k, both:]
    lse = top + jnp.log(total)
    lse_out[...] = lse
    per_cohort = scale / row_to_column(rest[1:2])
    weight_out[...] = jnp.broadcast_to(per_cohort, weight_out.shape)
    weights = jnp.zeros((both, LANES), F32)
    cohorts = jnp.concatenate([coh_near[...], coh_far[...]], axis=0)
    for c in range(NCOH):
        weights = jnp.where(cohorts == F32(c), per_cohort[c : c + 1, :], weights)
    loss = jnp.sum(weights * lse, keepdims=True)
    loss -= jnp.sum(per_cohort * row_to_column(rest[0:1]), keepdims=True)
    loss_out[...] = jnp.broadcast_to(loss, loss_out.shape)


def backward_core(rows, half, packed, bank, lse, weight, user_part, total):
    shards = packed.shape[0]
    bank_t = bank[...].T
    first = first_item(bank.shape[0])
    for at in range(0, shards, STEP):
        users = shard_users(packed, at, rows)
        logits = scores(bank[...], users)
        pos = local_positives(packed, at, rows, first)
        mine = cohort_row(packed, at, rows, 0)
        ids = iota((NCOH, mine.shape[1]), 0).astype(F32)
        weights = jnp.sum(jnp.where(ids == mine, weight[:, 0:1], F32(0)), axis=0, keepdims=True)
        line = half * shards + at
        level = jnp.concatenate([lse[line + s : line + s + 1, :] for s in range(STEP)], axis=1)
        hot = jnp.where(iota(logits.shape, 0) == pos, F32(1), F32(0))
        dlogits = (weights * (jnp.exp(logits - level) - hot)).astype(BF16)
        part = jnp.dot(bank_t, dlogits, preferred_element_type=F32).astype(BF16)
        for s in range(STEP):
            user_part[at + s] = part[:, s * LANES : (s + 1) * LANES]
        grad = jnp.dot(dlogits, users, preferred_element_type=F32)
        total = grad if total is None else total + grad
    return total


def backward_far_kernel(rows, scale, packed, bank, stats, coh_near, coh_far, *outs):
    user_part, bank_part, lse, weight, loss = outs
    settle(scale, stats, coh_near, coh_far, lse, weight, loss)
    bank_part[...] = backward_core(rows, 1, packed, bank, lse, weight, user_part, None)


def digits_of(value):
    high = value.astype(BF16)
    rest = value - high.astype(F32)
    mid = rest.astype(BF16)
    low = (rest - mid.astype(F32)).astype(BF16)
    row = iota(value.shape, 0)
    zero = F32(0)
    tile = jnp.where(row == 0, high.astype(F32), zero)
    tile = jnp.where(row == 1, mid.astype(F32), tile)
    return jnp.where(row == 2, low.astype(F32), tile).astype(BF16)


def read_digits(tile):
    return jnp.sum(tile.astype(F32), axis=0, keepdims=True)[:, :LANES]


def write_digits(out, at, value):
    tile = digits_of(jnp.broadcast_to(value, (8, LANES)))
    out[at : at + 8, :LANES] = tile
    out[at : at + 8, LANES:] = tile


def backward_near_kernel(rows, packed, bank, lse, weight, far_part, loss, user_part, out, acc):
    acc[...] = backward_core(rows, 0, packed, bank, lse, weight, user_part, far_part[...])
    nx, nc = lax.axis_size("x"), lax.axis_size("c")
    height = acc.shape[0] // (nx * nc)
    core = lax.axis_index("c")
    for side, owner in enumerate((1 - core, core)):
        for r in range(nx):
            piece = (lax.axis_index("x") + r) % nx * nc + owner
            at = pl.multiple_of(piece * height, height)
            to = side * (nx * height + 8) + r * height
            out[to : to + height, :] = acc[pl.ds(at, height), :].astype(BF16)
    write_digits(out, nx * height, loss[...])


def halve_kernel(mine, theirs, *pieces):
    below = theirs.shape[0]
    height = (below - 8) // len(pieces)
    loss = read_digits(mine[below - 8 : below, :]) + read_digits(theirs[below - 8 :, :])
    for r, piece in enumerate(pieces):
        cut = slice(below + r * height, below + (r + 1) * height)
        own = mine[cut, :].astype(F32) + theirs[r * height : (r + 1) * height, :].astype(F32)
        piece[:height, :] = own.astype(BF16)
        write_digits(piece, height, loss)


def gather_kernel(share, *refs):
    pieces, (grad, loss) = refs[:-2], refs[-2:]
    height = grad.shape[0]
    total = pieces[0][...].astype(F32)
    for piece in pieces[1:]:
        total = total + piece[...].astype(F32)
    grad[...] = total[:height]
    loss[...] = jnp.sum(total[height:], axis=0, keepdims=True)[:, :LANES] * share


def step(users, bank, positives, cohorts):
    rows, width = users.shape
    ny, nz, nx, nc = (lax.axis_size(a) for a in ALL)
    plane = ny * nx
    total_users = rows * plane * nz * nc
    cross = [(k, 1 - k) for k in range(nc)]

    cols = nx * nc
    fetch = [
        (((z + SHIFT[k]) % nz) * cols + k, z * cols + k) for z in range(nz) for k in range(cols)
    ]
    packed, count = call(
        pack_kernel,
        (bf16(plane, rows + 8, width), f32(8, LANES)),
        *(users, positives[None], cohorts[None]),
        limit=None,
    )
    near = exchange(packed, PLANE)
    item_block = lax.ppermute(bank, COLUMN, fetch)
    for axis, by in (("z", 1), ("z", 2), ("z", 4), ("c", 1)):
        ways = [(k, k ^ by) for k in range(lax.axis_size(axis))]
        count = count + lax.ppermute(count, axis, ways)
    far = lax.ppermute(near, "c", cross)

    near_stats, near_coh = forward(near, item_block, rows)
    other_near = lax.ppermute(near_stats, "c", cross)
    far_stats, far_coh = forward(far, item_block, rows)
    other_far = lax.ppermute(far_stats, "c", cross)
    stats = call(
        join_kernel,
        f32(plane, 2 * plane + 8, LANES),
        *(near_stats, far_stats, other_near, other_far, count),
    )
    stats = exchange(stats, PLANE)

    far_part, bank_part, lse, weight, loss = call(
        functools.partial(backward_far_kernel, rows, total_users / NCOH),
        (
            bf16(plane, width, rows),
            f32(*bank.shape),
            f32(2 * plane, LANES),
            f32(NCOH, LANES),
            f32(8, LANES),
        ),
        *(far, item_block, stats, near_coh, far_coh),
    )
    far_part = lax.ppermute(far_part, "c", cross)
    near_part, bank_part = call(
        functools.partial(backward_near_kernel, rows),
        (bf16(plane, width, rows), bf16(bank.shape[0] + 8, width)),
        *(near, item_block, lse, weight, bank_part, loss),
        scratch=[pltpu.VMEM(bank.shape, F32)],
    )
    bank_part = lax.ppermute(bank_part, COLUMN, [(b, a) for a, b in fetch])
    user_part = near_part + far_part
    user_part = exchange(user_part, PLANE)
    half = bank.shape[0] // nc
    height = half // nx
    theirs = lax.ppermute(bank_part[: half + 8], "c", cross)
    pieces = call(halve_kernel, (bf16(height + 8, width),) * nx, bank_part, theirs)
    arrived = [pieces[0]]
    for r in range(1, nx):
        arrived.append(lax.ppermute(pieces[r], "x", [(k, (k + r) % nx) for k in range(nx)]))
    bank_grad, loss = call(
        functools.partial(gather_kernel, 1.0 / total_users),
        (f32(height, width), f32(1, LANES)),
        *arrived,
    )
    user_grad = jnp.sum(user_part.astype(F32), axis=0).T
    return loss[0, 0], user_grad, bank_grad


def solution(mesh):
    torus = Mesh(mesh.devices.reshape(4, 8, 4, 2), ALL)
    return jax.shard_map(
        step,
        mesh=torus,
        in_specs=(P(ALL, None), P(("y", "z"), None), P(ALL), P(ALL)),
        out_specs=(P(), P(ALL, None), P(ALL, None)),
        check_vma=False,
    )
```

```python
import functools

import jax
import jax.numpy as jnp
from jax import lax
from jax.experimental import pallas as pl
from jax.experimental.pallas import tpu as pltpu
from jax.sharding import Mesh
from jax.sharding import PartitionSpec as P


NCOH = 16
PLANE = ("y", "x")
COLUMN = ("z", "x", "c")
ALL = ("y", "z", "x", "c")
SHIFT = (0, 4, 1, 5, 7, 3, 2, 6)
F32 = jnp.float32
BF16 = jnp.bfloat16
LANES = 128
RADIX = 128
STEP = 4
VMEM = pl.BlockSpec(memory_space=pltpu.VMEM)


def call(kernel, out_shape, *operands, scratch=(), limit=24 << 20):
    return pl.pallas_call(
        kernel,
        in_specs=[VMEM] * len(operands),
        out_specs=jax.tree.map(lambda _: VMEM, out_shape),
        out_shape=out_shape,
        scratch_shapes=list(scratch),
        compiler_params=pltpu.CompilerParams(vmem_limit_bytes=limit),
    )(*operands)


def f32(*shape):
    return jax.ShapeDtypeStruct(shape, F32)


def bf16(*shape):
    return jax.ShapeDtypeStruct(shape, BF16)


def first_item(items):
    column = lax.axis_index("x") * lax.axis_size("c") + lax.axis_index("c")
    shift = sum(jnp.where(column == k, by, 0) for k, by in enumerate(SHIFT))
    nz = lax.axis_size("z")
    return (lax.axis_index("y") * nz + (lax.axis_index("z") + shift) % nz) * items


def exchange(value, axis):
    return lax.all_to_all(value, axis, split_axis=0, concat_axis=0, tiled=True)


def scores(bank, users):
    return lax.dot_general(bank, users, (((1,), (1,)), ((), ())), preferred_element_type=F32)


def iota(shape, dim):
    return lax.broadcasted_iota(jnp.int32, shape, dim)


def shard_users(packed, at, rows):
    return jnp.concatenate([packed[at + s, :rows, :] for s in range(STEP)], axis=0)


def shard_row(packed, at, row, half):
    cut = slice(half * LANES, (half + 1) * LANES)
    tiles = [packed[at + s, row : row + 8, cut].astype(F32)[0:1] for s in range(STEP)]
    return jnp.concatenate(tiles, axis=1)


def cohort_row(packed, at, rows, half):
    cut = slice(half * LANES, (half + 1) * LANES)
    tiles = [packed[at + s, rows : rows + 8, cut].astype(F32)[1:2] for s in range(STEP)]
    return jnp.concatenate(tiles, axis=1)


def local_positives(packed, at, rows, first):
    high = shard_row(packed, at, rows, 0)
    low = shard_row(packed, at, rows, 1)
    return (high * RADIX + low).astype(jnp.int32) - first


def column_to_row(column):
    shape = (NCOH, LANES)
    spread = jnp.where(iota(shape, 0) == iota(shape, 1), column, F32(0))
    return jnp.sum(spread, axis=0, keepdims=True)


def row_to_column(row):
    shape = (NCOH, LANES)
    spread = jnp.where(iota(shape, 0) == iota(shape, 1), row, F32(0))
    return jnp.sum(spread, axis=1, keepdims=True)


def pack_kernel(users, positives, cohorts, out, count):
    rows, _ = users.shape
    pos = positives[...]
    high = (pos // RADIX).astype(F32)
    low = (pos % RADIX).astype(F32)
    mine = cohorts[...].astype(F32)
    row = iota((8, LANES), 0)
    left = jnp.where(row == 0, high, jnp.where(row == 1, mine, F32(0))).astype(BF16)
    right = jnp.where(row == 0, low, F32(0)).astype(BF16)
    for k in range(out.shape[0]):
        out[k, :rows, :] = users[...]
        out[k, rows:, :LANES] = left
        out[k, rows:, LANES:] = right
    ids = iota((NCOH, LANES), 0).astype(F32)
    column = jnp.sum(jnp.where(ids == mine, F32(1), F32(0)), axis=1, keepdims=True)
    count[...] = jnp.broadcast_to(column_to_row(column), (8, LANES))


def forward_kernel(rows, packed, bank, stats, coh):
    shards = packed.shape[0]
    first = first_item(bank.shape[0])
    positive = jnp.zeros((NCOH, 1), F32)
    for at in range(0, shards, STEP):
        logits = scores(bank[...], shard_users(packed, at, rows))
        top = jnp.max(logits, axis=0, keepdims=True)
        total = jnp.sum(jnp.exp(logits - top), axis=0, keepdims=True)
        pos = local_positives(packed, at, rows, first)
        own = jnp.sum(jnp.where(iota(logits.shape, 0) == pos, logits, F32(0)), axis=0, keepdims=True)
        lse = top + jnp.log(total)
        mine = cohort_row(packed, at, rows, 0)
        ids = iota((NCOH, mine.shape[1]), 0).astype(F32)
        positive += jnp.sum(jnp.where(ids == mine, own, F32(0)), axis=1, keepdims=True)
        for s in range(STEP):
            cut = slice(s * LANES, (s + 1) * LANES)
            stats[at + s : at + s + 1, :] = lse[:, cut]
            coh[at + s : at + s + 1, :] = mine[:, cut]
    stats[shards:, :] = jnp.broadcast_to(column_to_row(positive), (8, LANES))


def forward(packed, bank, rows):
    shards = packed.shape[0]
    shapes = (f32(shards + 8, LANES), f32(shards, LANES))
    return call(functools.partial(forward_kernel, rows), shapes, packed, bank)


def join_kernel(near, far, other_near, other_far, count, other_count, out):
    shards = near.shape[0] - 8

    def join(a, b):
        top = jnp.maximum(a, b)
        return top + jnp.log(jnp.exp(a - top) + jnp.exp(b - top))

    first = join(near[:shards], other_far[:shards])
    second = join(far[:shards], other_near[:shards])
    positive = near[shards:] + far[shards:] + other_near[shards:] + other_far[shards:]
    extra = jnp.where(iota(positive.shape, 0) == 0, positive, count[...] + other_count[...])
    for k in range(out.shape[0]):
        out[k, :shards] = first
        out[k, shards : 2 * shards] = second
        out[k, 2 * shards :] = extra


def settle(scale, stats, coh_near, coh_far, lse_out, weight_out, loss_out):
    shards = coh_near.shape[0]
    both = 2 * shards
    top = stats[0, :both]
    for k in range(1, stats.shape[0]):
        top = jnp.maximum(top, stats[k, :both])
    total = jnp.exp(stats[0, :both] - top)
    rest = stats[0, both:]
    for k in range(1, stats.shape[0]):
        total += jnp.exp(stats[k, :both] - top)
        rest += stats[k, both:]
    lse = top + jnp.log(total)
    lse_out[...] = lse
    per_cohort = scale / row_to_column(rest[1:2])
    weight_out[...] = jnp.broadcast_to(per_cohort, weight_out.shape)
    weights = jnp.zeros((both, LANES), F32)
    cohorts = jnp.concatenate([coh_near[...], coh_far[...]], axis=0)
    for c in range(NCOH):
        weights = jnp.where(cohorts == F32(c), per_cohort[c : c + 1, :], weights)
    loss = jnp.sum(weights * lse, keepdims=True)
    loss -= jnp.sum(per_cohort * row_to_column(rest[0:1]), keepdims=True)
    loss_out[...] = jnp.broadcast_to(loss, loss_out.shape)


def dlogits_at(rows, half, at, packed, bank, lse, weight):
    shards = packed.shape[0]
    users = shard_users(packed, at, rows)
    logits = scores(bank[...], users)
    pos = local_positives(packed, at, rows, first_item(bank.shape[0]))
    mine = cohort_row(packed, at, rows, 0)
    ids = iota((NCOH, mine.shape[1]), 0).astype(F32)
    weights = jnp.sum(jnp.where(ids == mine, weight[:, 0:1], F32(0)), axis=0, keepdims=True)
    line = half * shards + at
    level = jnp.concatenate([lse[line + s : line + s + 1, :] for s in range(STEP)], axis=1)
    hot = jnp.where(iota(logits.shape, 0) == pos, F32(1), F32(0))
    return users, (weights * (jnp.exp(logits - level) - hot)).astype(BF16)


def backward_far_kernel(rows, scale, packed, bank, stats, coh_near, coh_far, *outs):
    user_part, bank_part, lse, weight, loss = outs
    settle(scale, stats, coh_near, coh_far, lse, weight, loss)
    bank_t = bank[...].T
    total = None
    for at in range(0, packed.shape[0], STEP):
        users, dlogits = dlogits_at(rows, 1, at, packed, bank, lse, weight)
        part = jnp.dot(bank_t, dlogits, preferred_element_type=F32).astype(BF16)
        for s in range(STEP):
            user_part[at + s] = part[:, s * LANES : (s + 1) * LANES]
        grad = jnp.dot(dlogits, users, preferred_element_type=F32)
        total = grad if total is None else total + grad
    bank_part[...] = total


def digits_of(value):
    high = value.astype(BF16)
    rest = value - high.astype(F32)
    mid = rest.astype(BF16)
    low = (rest - mid.astype(F32)).astype(BF16)
    row = iota(value.shape, 0)
    zero = F32(0)
    tile = jnp.where(row == 0, high.astype(F32), zero)
    tile = jnp.where(row == 1, mid.astype(F32), tile)
    return jnp.where(row == 2, low.astype(F32), tile).astype(BF16)


def read_digits(tile):
    return jnp.sum(tile.astype(F32), axis=0, keepdims=True)[:, :LANES]


def write_digits(out, at, value):
    tile = digits_of(jnp.broadcast_to(value, (8, LANES)))
    out[at : at + 8, :LANES] = tile
    out[at : at + 8, LANES:] = tile


def backward_near_kernel(rows, packed, bank, lse, weight, far_part, loss, kept, out, acc):
    total = far_part[...]
    for step in range(packed.shape[0] // STEP):
        users, dlogits = dlogits_at(rows, 0, step * STEP, packed, bank, lse, weight)
        kept[step] = dlogits
        total = total + jnp.dot(dlogits, users, preferred_element_type=F32)
    acc[...] = total
    nx, nc = lax.axis_size("x"), lax.axis_size("c")
    height = acc.shape[0] // (nx * nc)
    core = lax.axis_index("c")
    for side, owner in enumerate((1 - core, core)):
        for r in range(nx):
            piece = (lax.axis_index("x") + r) % nx * nc + owner
            at = pl.multiple_of(piece * height, height)
            to = side * (nx * height + 8) + r * height
            out[to : to + height, :] = acc[pl.ds(at, height), :].astype(BF16)
    write_digits(out, nx * height, loss[...])


def users_near_kernel(kept, bank, far_part, user_part):
    bank_t = bank[...].T
    for step in range(kept.shape[0]):
        part = jnp.dot(bank_t, kept[step], preferred_element_type=F32)
        for s in range(STEP):
            mine = part[:, s * LANES : (s + 1) * LANES]
            at = step * STEP + s
            user_part[at] = (mine + far_part[at].astype(F32)).astype(BF16)


def finish_kernel(parts, out):
    total = parts[0].astype(F32)
    for k in range(1, parts.shape[0]):
        total = total + parts[k].astype(F32)
    out[...] = total.T


def halve_kernel(mine, theirs, *pieces):
    below = theirs.shape[0]
    height = (below - 8) // len(pieces)
    loss = read_digits(mine[below - 8 : below, :]) + read_digits(theirs[below - 8 :, :])
    for r, piece in enumerate(pieces):
        cut = slice(below + r * height, below + (r + 1) * height)
        own = mine[cut, :].astype(F32) + theirs[r * height : (r + 1) * height, :].astype(F32)
        piece[:height, :] = own.astype(BF16)
        write_digits(piece, height, loss)


def gather_kernel(share, *refs):
    pieces, (grad, loss) = refs[:-2], refs[-2:]
    height = grad.shape[0]
    total = pieces[0][...].astype(F32)
    for piece in pieces[1:]:
        total = total + piece[...].astype(F32)
    grad[...] = total[:height]
    loss[...] = jnp.sum(total[height:], axis=0, keepdims=True)[:, :LANES] * share


def step(users, bank, positives, cohorts):
    rows, width = users.shape
    ny, nz, nx, nc = (lax.axis_size(a) for a in ALL)
    plane = ny * nx
    total_users = rows * plane * nz * nc
    cross = [(k, 1 - k) for k in range(nc)]

    cols = nx * nc
    fetch = [
        (((z + SHIFT[k]) % nz) * cols + k, z * cols + k) for z in range(nz) for k in range(cols)
    ]
    packed, count = call(
        pack_kernel,
        (bf16(plane, rows + 8, width), f32(8, LANES)),
        *(users, positives[None], cohorts[None]),
        limit=None,
    )
    near = exchange(packed, PLANE)
    item_block = lax.ppermute(bank, COLUMN, fetch)
    for axis, by in (("c", 1), ("z", 1), ("z", 2), ("z", 4)):
        ways = [(k, k ^ by) for k in range(lax.axis_size(axis))]
        other_count = lax.ppermute(count, axis, ways)
        if by < 4:
            count = count + other_count
    far = lax.ppermute(near, "c", cross)

    near_stats, near_coh = forward(near, item_block, rows)
    other_near = lax.ppermute(near_stats, "c", cross)
    far_stats, far_coh = forward(far, item_block, rows)
    other_far = lax.ppermute(far_stats, "c", cross)
    stats = call(
        join_kernel,
        f32(plane, 2 * plane + 8, LANES),
        *(near_stats, far_stats, other_near, other_far, count, other_count),
    )
    stats = exchange(stats, PLANE)

    far_part, bank_part, lse, weight, loss = call(
        functools.partial(backward_far_kernel, rows, total_users / NCOH),
        (
            bf16(plane, width, rows),
            f32(*bank.shape),
            f32(2 * plane, LANES),
            f32(NCOH, LANES),
            f32(8, LANES),
        ),
        *(far, item_block, stats, near_coh, far_coh),
    )
    far_part = lax.ppermute(far_part, "c", cross)
    kept, bank_part = call(
        functools.partial(backward_near_kernel, rows),
        (bf16(plane // STEP, bank.shape[0], STEP * rows), bf16(bank.shape[0] + 8, width)),
        *(near, item_block, lse, weight, bank_part, loss),
        scratch=[pltpu.VMEM(bank.shape, F32)],
    )
    bank_part = lax.ppermute(bank_part, COLUMN, [(b, a) for a, b in fetch])
    user_part = call(users_near_kernel, bf16(plane, width, rows), *(kept, item_block, far_part))
    user_part = exchange(user_part, PLANE)
    half = bank.shape[0] // nc
    height = half // nx
    theirs = lax.ppermute(bank_part[: half + 8], "c", cross)
    pieces = call(halve_kernel, (bf16(height + 8, width),) * nx, bank_part, theirs)
    arrived = [pieces[0]]
    for r in range(1, nx):
        arrived.append(lax.ppermute(pieces[r], "x", [(k, (k + r) % nx) for k in range(nx)]))
    user_grad = call(finish_kernel, f32(rows, width), user_part)
    user_grad, *arrived = lax.optimization_barrier((user_grad, *arrived))
    bank_grad, loss = call(
        functools.partial(gather_kernel, 1.0 / total_users),
        (f32(height, width), f32(1, LANES)),
        *arrived,
    )
    return loss[0, 0], user_grad, bank_grad


def solution(mesh):
    torus = Mesh(mesh.devices.reshape(4, 8, 4, 2), ALL)
    return jax.shard_map(
        step,
        mesh=torus,
        in_specs=(P(ALL, None), P(("y", "z"), None), P(ALL), P(ALL)),
        out_specs=(P(), P(ALL, None), P(ALL, None)),
        check_vma=False,
    )
```

```python
import functools

import jax
import jax.numpy as jnp
from jax import lax
from jax.experimental import pallas as pl
from jax.experimental.pallas import tpu as pltpu
from jax.sharding import Mesh
from jax.sharding import PartitionSpec as P


NCOH = 16
PLANE = ("y", "x")
COLUMN = ("z", "x", "c")
ALL = ("y", "z", "x", "c")
SHIFT = (0, 4, 1, 5, 7, 3, 2, 6)
F32 = jnp.float32
BF16 = jnp.bfloat16
LANES = 128
RADIX = 128
STEP = 4
VMEM = pl.BlockSpec(memory_space=pltpu.VMEM)


def call(kernel, out_shape, *operands, scratch=(), limit=24 << 20):
    return pl.pallas_call(
        kernel,
        in_specs=[VMEM] * len(operands),
        out_specs=jax.tree.map(lambda _: VMEM, out_shape),
        out_shape=out_shape,
        scratch_shapes=list(scratch),
        compiler_params=pltpu.CompilerParams(vmem_limit_bytes=limit),
    )(*operands)


def f32(*shape):
    return jax.ShapeDtypeStruct(shape, F32)


def bf16(*shape):
    return jax.ShapeDtypeStruct(shape, BF16)


def first_item(items):
    column = lax.axis_index("x") * lax.axis_size("c") + lax.axis_index("c")
    shift = sum(jnp.where(column == k, by, 0) for k, by in enumerate(SHIFT))
    nz = lax.axis_size("z")
    return (lax.axis_index("y") * nz + (lax.axis_index("z") + shift) % nz) * items


def exchange(value, axis):
    return lax.all_to_all(value, axis, split_axis=0, concat_axis=0, tiled=True)


def scores(bank, users):
    return lax.dot_general(bank, users, (((1,), (1,)), ((), ())), preferred_element_type=F32)


def iota(shape, dim):
    return lax.broadcasted_iota(jnp.int32, shape, dim)


def shard_users(packed, at, rows):
    return jnp.concatenate([packed[at + s, :rows, :] for s in range(STEP)], axis=0)


def shard_row(packed, at, row, half):
    cut = slice(half * LANES, (half + 1) * LANES)
    tiles = [packed[at + s, row : row + 8, cut].astype(F32)[0:1] for s in range(STEP)]
    return jnp.concatenate(tiles, axis=1)


def cohort_row(packed, at, rows, half):
    cut = slice(half * LANES, (half + 1) * LANES)
    tiles = [packed[at + s, rows : rows + 8, cut].astype(F32)[1:2] for s in range(STEP)]
    return jnp.concatenate(tiles, axis=1)


def local_positives(packed, at, rows, first):
    high = shard_row(packed, at, rows, 0)
    low = shard_row(packed, at, rows, 1)
    return (high * RADIX + low).astype(jnp.int32) - first


def column_to_row(column):
    shape = (NCOH, LANES)
    spread = jnp.where(iota(shape, 0) == iota(shape, 1), column, F32(0))
    return jnp.sum(spread, axis=0, keepdims=True)


def row_to_column(row):
    shape = (NCOH, LANES)
    spread = jnp.where(iota(shape, 0) == iota(shape, 1), row, F32(0))
    return jnp.sum(spread, axis=1, keepdims=True)


def pack_kernel(users, positives, cohorts, out, count):
    rows, _ = users.shape
    pos = positives[...]
    high = (pos // RADIX).astype(F32)
    low = (pos % RADIX).astype(F32)
    mine = cohorts[...].astype(F32)
    row = iota((8, LANES), 0)
    left = jnp.where(row == 0, high, jnp.where(row == 1, mine, F32(0))).astype(BF16)
    right = jnp.where(row == 0, low, F32(0)).astype(BF16)
    for k in range(out.shape[0]):
        out[k, :rows, :] = users[...]
        out[k, rows:, :LANES] = left
        out[k, rows:, LANES:] = right
    ids = iota((NCOH, LANES), 0).astype(F32)
    column = jnp.sum(jnp.where(ids == mine, F32(1), F32(0)), axis=1, keepdims=True)
    count[...] = jnp.broadcast_to(column_to_row(column), (8, LANES))


def forward_kernel(rows, packed, bank, stats, coh):
    shards = packed.shape[0]
    first = first_item(bank.shape[0])
    positive = jnp.zeros((NCOH, 1), F32)
    for at in range(0, shards, STEP):
        logits = scores(bank[...], shard_users(packed, at, rows))
        top = jnp.max(logits, axis=0, keepdims=True)
        total = jnp.sum(jnp.exp(logits - top), axis=0, keepdims=True)
        pos = local_positives(packed, at, rows, first)
        own = jnp.sum(jnp.where(iota(logits.shape, 0) == pos, logits, F32(0)), axis=0, keepdims=True)
        lse = top + jnp.log(total)
        mine = cohort_row(packed, at, rows, 0)
        ids = iota((NCOH, mine.shape[1]), 0).astype(F32)
        positive += jnp.sum(jnp.where(ids == mine, own, F32(0)), axis=1, keepdims=True)
        for s in range(STEP):
            cut = slice(s * LANES, (s + 1) * LANES)
            stats[at + s : at + s + 1, :] = lse[:, cut]
            coh[at + s : at + s + 1, :] = mine[:, cut]
    stats[shards:, :] = jnp.broadcast_to(column_to_row(positive), (8, LANES))


def forward(packed, bank, rows):
    shards = packed.shape[0]
    shapes = (f32(shards + 8, LANES), f32(shards, LANES))
    return call(functools.partial(forward_kernel, rows), shapes, packed, bank)


def join_kernel(near, far, other_near, other_far, count, other_count, out):
    shards = near.shape[0] - 8

    def join(a, b):
        top = jnp.maximum(a, b)
        return top + jnp.log(jnp.exp(a - top) + jnp.exp(b - top))

    first = join(near[:shards], other_far[:shards])
    second = join(far[:shards], other_near[:shards])
    positive = near[shards:] + far[shards:] + other_near[shards:] + other_far[shards:]
    extra = jnp.where(iota(positive.shape, 0) == 0, positive, count[...] + other_count[...])
    for k in range(out.shape[0]):
        out[k, :shards] = first
        out[k, shards : 2 * shards] = second
        out[k, 2 * shards :] = extra


def settle(scale, stats, coh_near, coh_far, lse_out, weight_out, loss_out):
    shards = coh_near.shape[0]
    both = 2 * shards
    top = stats[0, :both]
    for k in range(1, stats.shape[0]):
        top = jnp.maximum(top, stats[k, :both])
    total = jnp.exp(stats[0, :both] - top)
    rest = stats[0, both:]
    for k in range(1, stats.shape[0]):
        total += jnp.exp(stats[k, :both] - top)
        rest += stats[k, both:]
    lse = top + jnp.log(total)
    lse_out[...] = lse
    per_cohort = scale / row_to_column(rest[1:2])
    weight_out[...] = jnp.broadcast_to(per_cohort, weight_out.shape)
    weights = jnp.zeros((both, LANES), F32)
    cohorts = jnp.concatenate([coh_near[...], coh_far[...]], axis=0)
    for c in range(NCOH):
        weights = jnp.where(cohorts == F32(c), per_cohort[c : c + 1, :], weights)
    loss = jnp.sum(weights * lse, keepdims=True)
    loss -= jnp.sum(per_cohort * row_to_column(rest[0:1]), keepdims=True)
    loss_out[...] = jnp.broadcast_to(loss, loss_out.shape)


def dlogits_at(rows, half, at, packed, bank, lse, weight):
    shards = packed.shape[0]
    users = shard_users(packed, at, rows)
    logits = scores(bank[...], users)
    pos = local_positives(packed, at, rows, first_item(bank.shape[0]))
    mine = cohort_row(packed, at, rows, 0)
    ids = iota((NCOH, mine.shape[1]), 0).astype(F32)
    weights = jnp.sum(jnp.where(ids == mine, weight[:, 0:1], F32(0)), axis=0, keepdims=True)
    line = half * shards + at
    level = jnp.concatenate([lse[line + s : line + s + 1, :] for s in range(STEP)], axis=1)
    hot = jnp.where(iota(logits.shape, 0) == pos, F32(1), F32(0))
    return users, (weights * (jnp.exp(logits - level) - hot)).astype(BF16)


def backward_far_kernel(rows, scale, packed, bank, stats, coh_near, coh_far, *outs):
    user_part, bank_part, lse, weight, loss = outs
    settle(scale, stats, coh_near, coh_far, lse, weight, loss)
    bank_t = bank[...].T
    total = None
    for at in range(0, packed.shape[0], STEP):
        users, dlogits = dlogits_at(rows, 1, at, packed, bank, lse, weight)
        part = jnp.dot(bank_t, dlogits, preferred_element_type=F32).astype(BF16)
        for s in range(STEP):
            user_part[at + s] = part[:, s * LANES : (s + 1) * LANES]
        grad = jnp.dot(dlogits, users, preferred_element_type=F32)
        total = grad if total is None else total + grad
    bank_part[...] = total


def digits_of(value):
    high = value.astype(BF16)
    rest = value - high.astype(F32)
    mid = rest.astype(BF16)
    low = (rest - mid.astype(F32)).astype(BF16)
    row = iota(value.shape, 0)
    zero = F32(0)
    tile = jnp.where(row == 0, high.astype(F32), zero)
    tile = jnp.where(row == 1, mid.astype(F32), tile)
    return jnp.where(row == 2, low.astype(F32), tile).astype(BF16)


def read_digits(tile):
    return jnp.sum(tile.astype(F32), axis=0, keepdims=True)[:, :LANES]


def write_digits(out, at, value):
    tile = digits_of(jnp.broadcast_to(value, (8, LANES)))
    out[at : at + 8, :LANES] = tile
    out[at : at + 8, LANES:] = tile


def backward_near_kernel(rows, packed, bank, lse, weight, far_part, loss, kept, out, acc):
    total = far_part[...]
    for step in range(packed.shape[0] // STEP):
        users, dlogits = dlogits_at(rows, 0, step * STEP, packed, bank, lse, weight)
        kept[step] = dlogits
        total = total + jnp.dot(dlogits, users, preferred_element_type=F32)
    acc[...] = total
    nx, nc = lax.axis_size("x"), lax.axis_size("c")
    height = acc.shape[0] // (nx * nc)
    core = lax.axis_index("c")
    for side, owner in enumerate((1 - core, core)):
        for r in range(nx):
            piece = (lax.axis_index("x") + r) % nx * nc + owner
            at = pl.multiple_of(piece * height, height)
            to = side * (nx * height + 8) + r * height
            out[to : to + height, :] = acc[pl.ds(at, height), :].astype(BF16)
    write_digits(out, nx * height, loss[...])


def users_near_kernel(kept, bank, far_part, user_part):
    bank_t = bank[...].T
    for step in range(kept.shape[0]):
        part = jnp.dot(bank_t, kept[step], preferred_element_type=F32)
        for s in range(STEP):
            mine = part[:, s * LANES : (s + 1) * LANES]
            at = step * STEP + s
            user_part[at] = (mine + far_part[at].astype(F32)).astype(BF16)


def halve_kernel(mine, theirs, *pieces):
    below = theirs.shape[0]
    height = (below - 8) // len(pieces)
    loss = read_digits(mine[below - 8 : below, :]) + read_digits(theirs[below - 8 :, :])
    for r, piece in enumerate(pieces):
        cut = slice(below + r * height, below + (r + 1) * height)
        own = mine[cut, :].astype(F32) + theirs[r * height : (r + 1) * height, :].astype(F32)
        piece[:height, :] = own.astype(BF16)
        write_digits(piece, height, loss)


def finish_kernel(share, parts, *refs):
    pieces, (user_grad, bank_grad, loss) = refs[:-3], refs[-3:]
    total = parts[0].astype(F32)
    for k in range(1, parts.shape[0]):
        total = total + parts[k].astype(F32)
    user_grad[...] = total.T
    height = bank_grad.shape[0]
    total = pieces[0][...].astype(F32)
    for piece in pieces[1:]:
        total = total + piece[...].astype(F32)
    bank_grad[...] = total[:height]
    loss[...] = jnp.sum(total[height:], axis=0, keepdims=True)[:, :LANES] * share


def step(users, bank, positives, cohorts):
    rows, width = users.shape
    ny, nz, nx, nc = (lax.axis_size(a) for a in ALL)
    plane = ny * nx
    total_users = rows * plane * nz * nc
    cross = [(k, 1 - k) for k in range(nc)]

    cols = nx * nc
    fetch = [
        (((z + SHIFT[k]) % nz) * cols + k, z * cols + k) for z in range(nz) for k in range(cols)
    ]
    packed, count = call(
        pack_kernel,
        (bf16(plane, rows + 8, width), f32(8, LANES)),
        *(users, positives[None], cohorts[None]),
        limit=None,
    )
    near = exchange(packed, PLANE)
    item_block = lax.ppermute(bank, COLUMN, fetch)
    for axis, by in (("z", 4), ("z", 2), ("c", 1), ("z", 1)):
        ways = [(k, k ^ by) for k in range(lax.axis_size(axis))]
        other_count = lax.ppermute(count, axis, ways)
        if (axis, by) != ("z", 1):
            count = count + other_count
    far = lax.ppermute(near, "c", cross)

    near_stats, near_coh = forward(near, item_block, rows)
    other_near = lax.ppermute(near_stats, "c", cross)
    far_stats, far_coh = forward(far, item_block, rows)
    other_far = lax.ppermute(far_stats, "c", cross)
    stats = call(
        join_kernel,
        f32(plane, 2 * plane + 8, LANES),
        *(near_stats, far_stats, other_near, other_far, count, other_count),
    )
    stats = exchange(stats, PLANE)

    far_part, bank_part, lse, weight, loss = call(
        functools.partial(backward_far_kernel, rows, total_users / NCOH),
        (
            bf16(plane, width, rows),
            f32(*bank.shape),
            f32(2 * plane, LANES),
            f32(NCOH, LANES),
            f32(8, LANES),
        ),
        *(far, item_block, stats, near_coh, far_coh),
    )
    far_part = lax.ppermute(far_part, "c", cross)
    kept, bank_part = call(
        functools.partial(backward_near_kernel, rows),
        (bf16(plane // STEP, bank.shape[0], STEP * rows), bf16(bank.shape[0] + 8, width)),
        *(near, item_block, lse, weight, bank_part, loss),
        scratch=[pltpu.VMEM(bank.shape, F32)],
    )
    bank_part = lax.ppermute(bank_part, COLUMN, [(b, a) for a, b in fetch])
    user_part = call(users_near_kernel, bf16(plane, width, rows), *(kept, item_block, far_part))
    user_part = exchange(user_part, PLANE)
    half = bank.shape[0] // nc
    height = half // nx
    theirs = lax.ppermute(bank_part[: half + 8], "c", cross)
    pieces = call(halve_kernel, (bf16(height + 8, width),) * nx, bank_part, theirs)
    arrived = [pieces[0]]
    for r in range(1, nx):
        arrived.append(lax.ppermute(pieces[r], "x", [(k, (k + r) % nx) for k in range(nx)]))
    user_grad, bank_grad, loss = call(
        functools.partial(finish_kernel, 1.0 / total_users),
        (f32(rows, width), f32(height, width), f32(1, LANES)),
        *(user_part, *arrived),
    )
    return loss[0, 0], user_grad, bank_grad


def solution(mesh):
    torus = Mesh(mesh.devices.reshape(4, 8, 4, 2), ALL)
    return jax.shard_map(
        step,
        mesh=torus,
        in_specs=(P(ALL, None), P(("y", "z"), None), P(ALL), P(ALL)),
        out_specs=(P(), P(ALL, None), P(ALL, None)),
        check_vma=False,
    )
```

```python
import functools

import jax
import jax.numpy as jnp
from jax import lax
from jax.experimental import pallas as pl
from jax.experimental.pallas import tpu as pltpu
from jax.sharding import Mesh
from jax.sharding import PartitionSpec as P


NCOH = 16
PLANE = ("y", "x")
COLUMN = ("z", "x", "c")
ALL = ("y", "z", "x", "c")
SHIFT = (0, 4, 1, 5, 7, 3, 2, 6)
F32 = jnp.float32
BF16 = jnp.bfloat16
LANES = 128
RADIX = 128
STEP = 4
VMEM = pl.BlockSpec(memory_space=pltpu.VMEM)


def call(kernel, out_shape, *operands, scratch=(), limit=24 << 20):
    return pl.pallas_call(
        kernel,
        in_specs=[VMEM] * len(operands),
        out_specs=jax.tree.map(lambda _: VMEM, out_shape),
        out_shape=out_shape,
        scratch_shapes=list(scratch),
        compiler_params=pltpu.CompilerParams(vmem_limit_bytes=limit),
    )(*operands)


def f32(*shape):
    return jax.ShapeDtypeStruct(shape, F32)


def bf16(*shape):
    return jax.ShapeDtypeStruct(shape, BF16)


def first_item(items):
    column = lax.axis_index("x") * lax.axis_size("c") + lax.axis_index("c")
    shift = sum(jnp.where(column == k, by, 0) for k, by in enumerate(SHIFT))
    nz = lax.axis_size("z")
    return (lax.axis_index("y") * nz + (lax.axis_index("z") + shift) % nz) * items


def exchange(value, axis):
    return lax.all_to_all(value, axis, split_axis=0, concat_axis=0, tiled=True)


def scores(bank, users):
    return lax.dot_general(bank, users, (((1,), (1,)), ((), ())), preferred_element_type=F32)


def iota(shape, dim):
    return lax.broadcasted_iota(jnp.int32, shape, dim)


def shard_users(packed, at, rows):
    return jnp.concatenate([packed[at + s, :rows, :] for s in range(STEP)], axis=0)


def shard_row(packed, at, row, half):
    cut = slice(half * LANES, (half + 1) * LANES)
    tiles = [packed[at + s, row : row + 8, cut].astype(F32)[0:1] for s in range(STEP)]
    return jnp.concatenate(tiles, axis=1)


def cohort_row(packed, at, rows, half):
    cut = slice(half * LANES, (half + 1) * LANES)
    tiles = [packed[at + s, rows : rows + 8, cut].astype(F32)[1:2] for s in range(STEP)]
    return jnp.concatenate(tiles, axis=1)


def local_positives(packed, at, rows, first):
    high = shard_row(packed, at, rows, 0)
    low = shard_row(packed, at, rows, 1)
    return (high * RADIX + low).astype(jnp.int32) - first


def column_to_row(column):
    shape = (NCOH, LANES)
    spread = jnp.where(iota(shape, 0) == iota(shape, 1), column, F32(0))
    return jnp.sum(spread, axis=0, keepdims=True)


def row_to_column(row):
    shape = (NCOH, LANES)
    spread = jnp.where(iota(shape, 0) == iota(shape, 1), row, F32(0))
    return jnp.sum(spread, axis=1, keepdims=True)


def pack_kernel(users, positives, cohorts, out, count):
    rows, _ = users.shape
    pos = positives[...]
    high = (pos // RADIX).astype(F32)
    low = (pos % RADIX).astype(F32)
    mine = cohorts[...].astype(F32)
    row = iota((8, LANES), 0)
    left = jnp.where(row == 0, high, jnp.where(row == 1, mine, F32(0))).astype(BF16)
    right = jnp.where(row == 0, low, F32(0)).astype(BF16)
    for k in range(out.shape[0]):
        out[k, :rows, :] = users[...]
        out[k, rows:, :LANES] = left
        out[k, rows:, LANES:] = right
    ids = iota((NCOH, LANES), 0).astype(F32)
    column = jnp.sum(jnp.where(ids == mine, F32(1), F32(0)), axis=1, keepdims=True)
    count[...] = jnp.broadcast_to(column_to_row(column), (8, LANES))


def forward_kernel(rows, packed, bank, stats, coh):
    shards = packed.shape[0]
    first = first_item(bank.shape[0])
    positive = jnp.zeros((NCOH, 1), F32)
    for at in range(0, shards, STEP):
        logits = scores(bank[...], shard_users(packed, at, rows))
        top = jnp.max(logits, axis=0, keepdims=True)
        total = jnp.sum(jnp.exp(logits - top), axis=0, keepdims=True)
        pos = local_positives(packed, at, rows, first)
        own = jnp.sum(jnp.where(iota(logits.shape, 0) == pos, logits, F32(0)), axis=0, keepdims=True)
        lse = top + jnp.log(total)
        mine = cohort_row(packed, at, rows, 0)
        ids = iota((NCOH, mine.shape[1]), 0).astype(F32)
        positive += jnp.sum(jnp.where(ids == mine, own, F32(0)), axis=1, keepdims=True)
        for s in range(STEP):
            cut = slice(s * LANES, (s + 1) * LANES)
            stats[at + s : at + s + 1, :] = lse[:, cut]
            coh[at + s : at + s + 1, :] = mine[:, cut]
    stats[shards:, :] = jnp.broadcast_to(column_to_row(positive), (8, LANES))


def forward(packed, bank, rows):
    shards = packed.shape[0]
    shapes = (f32(shards + 8, LANES), f32(shards, LANES))
    return call(functools.partial(forward_kernel, rows), shapes, packed, bank)


def join_kernel(near, far, other_near, other_far, count, other_count, out):
    shards = near.shape[0] - 8

    def join(a, b):
        top = jnp.maximum(a, b)
        return top + jnp.log(jnp.exp(a - top) + jnp.exp(b - top))

    first = join(near[:shards], other_far[:shards])
    second = join(far[:shards], other_near[:shards])
    positive = near[shards:] + far[shards:] + other_near[shards:] + other_far[shards:]
    extra = jnp.where(iota(positive.shape, 0) == 0, positive, count[...] + other_count[...])
    for k in range(out.shape[0]):
        out[k, :shards] = first
        out[k, shards : 2 * shards] = second
        out[k, 2 * shards :] = extra


def settle(scale, stats, coh_near, coh_far, lse_out, weight_out, loss_out):
    shards = coh_near.shape[0]
    both = 2 * shards
    top = stats[0, :both]
    for k in range(1, stats.shape[0]):
        top = jnp.maximum(top, stats[k, :both])
    total = jnp.exp(stats[0, :both] - top)
    rest = stats[0, both:]
    for k in range(1, stats.shape[0]):
        total += jnp.exp(stats[k, :both] - top)
        rest += stats[k, both:]
    lse = top + jnp.log(total)
    lse_out[...] = lse
    counts = row_to_column(rest[1:2])
    per_cohort = jnp.where(counts > 0, scale / jnp.maximum(counts, F32(1)), F32(0))
    weight_out[...] = jnp.broadcast_to(per_cohort, weight_out.shape)
    weights = jnp.zeros((both, LANES), F32)
    cohorts = jnp.concatenate([coh_near[...], coh_far[...]], axis=0)
    for c in range(NCOH):
        weights = jnp.where(cohorts == F32(c), per_cohort[c : c + 1, :], weights)
    loss = jnp.sum(weights * lse, keepdims=True)
    loss -= jnp.sum(per_cohort * row_to_column(rest[0:1]), keepdims=True)
    loss_out[...] = jnp.broadcast_to(loss, loss_out.shape)


def dlogits_at(rows, half, at, packed, bank, lse, weight):
    shards = packed.shape[0]
    users = shard_users(packed, at, rows)
    logits = scores(bank[...], users)
    pos = local_positives(packed, at, rows, first_item(bank.shape[0]))
    mine = cohort_row(packed, at, rows, 0)
    ids = iota((NCOH, mine.shape[1]), 0).astype(F32)
    weights = jnp.sum(jnp.where(ids == mine, weight[:, 0:1], F32(0)), axis=0, keepdims=True)
    line = half * shards + at
    level = jnp.concatenate([lse[line + s : line + s + 1, :] for s in range(STEP)], axis=1)
    hot = jnp.where(iota(logits.shape, 0) == pos, F32(1), F32(0))
    return users, (weights * (jnp.exp(logits - level) - hot)).astype(BF16)


def backward_far_kernel(rows, scale, packed, bank, stats, coh_near, coh_far, *outs):
    user_part, bank_part, lse, weight, loss = outs
    settle(scale, stats, coh_near, coh_far, lse, weight, loss)
    bank_t = bank[...].T
    total = None
    for at in range(0, packed.shape[0], STEP):
        users, dlogits = dlogits_at(rows, 1, at, packed, bank, lse, weight)
        part = jnp.dot(bank_t, dlogits, preferred_element_type=F32).astype(BF16)
        for s in range(STEP):
            user_part[at + s] = part[:, s * LANES : (s + 1) * LANES]
        grad = jnp.dot(dlogits, users, preferred_element_type=F32)
        total = grad if total is None else total + grad
    bank_part[...] = total


def digits_of(value):
    high = value.astype(BF16)
    rest = value - high.astype(F32)
    mid = rest.astype(BF16)
    low = (rest - mid.astype(F32)).astype(BF16)
    row = iota(value.shape, 0)
    zero = F32(0)
    tile = jnp.where(row == 0, high.astype(F32), zero)
    tile = jnp.where(row == 1, mid.astype(F32), tile)
    return jnp.where(row == 2, low.astype(F32), tile).astype(BF16)


def read_digits(tile):
    return jnp.sum(tile.astype(F32), axis=0, keepdims=True)[:, :LANES]


def write_digits(out, at, value):
    tile = digits_of(jnp.broadcast_to(value, (8, LANES)))
    out[at : at + 8, :LANES] = tile
    out[at : at + 8, LANES:] = tile


def backward_near_kernel(rows, packed, bank, lse, weight, far_part, loss, kept, out, acc):
    total = far_part[...]
    for step in range(packed.shape[0] // STEP):
        users, dlogits = dlogits_at(rows, 0, step * STEP, packed, bank, lse, weight)
        kept[step] = dlogits
        total = total + jnp.dot(dlogits, users, preferred_element_type=F32)
    acc[...] = total
    nx, nc = lax.axis_size("x"), lax.axis_size("c")
    height = acc.shape[0] // (nx * nc)
    core = lax.axis_index("c")
    for side, owner in enumerate((1 - core, core)):
        for r in range(nx):
            piece = (lax.axis_index("x") + r) % nx * nc + owner
            at = pl.multiple_of(piece * height, height)
            to = side * (nx * height + 8) + r * height
            out[to : to + height, :] = acc[pl.ds(at, height), :].astype(BF16)
    write_digits(out, nx * height, loss[...])


def users_near_kernel(kept, bank, far_part, user_part):
    bank_t = bank[...].T
    for step in range(kept.shape[0]):
        part = jnp.dot(bank_t, kept[step], preferred_element_type=F32)
        for s in range(STEP):
            mine = part[:, s * LANES : (s + 1) * LANES]
            at = step * STEP + s
            user_part[at] = (mine + far_part[at].astype(F32)).astype(BF16)


def halve_kernel(mine, theirs, *pieces):
    below = theirs.shape[0]
    height = (below - 8) // len(pieces)
    loss = read_digits(mine[below - 8 : below, :]) + read_digits(theirs[below - 8 :, :])
    for r, piece in enumerate(pieces):
        cut = slice(below + r * height, below + (r + 1) * height)
        own = mine[cut, :].astype(F32) + theirs[r * height : (r + 1) * height, :].astype(F32)
        piece[:height, :] = own.astype(BF16)
        write_digits(piece, height, loss)


def finish_kernel(share, parts, *refs):
    pieces, (user_grad, bank_grad, loss) = refs[:-3], refs[-3:]
    total = parts[0].astype(F32)
    for k in range(1, parts.shape[0]):
        total = total + parts[k].astype(F32)
    user_grad[...] = total.T
    height = bank_grad.shape[0]
    total = pieces[0][...].astype(F32)
    for piece in pieces[1:]:
        total = total + piece[...].astype(F32)
    bank_grad[...] = total[:height]
    loss[...] = jnp.sum(total[height:], axis=0, keepdims=True)[:, :LANES] * share


def step(users, bank, positives, cohorts):
    rows, width = users.shape
    ny, nz, nx, nc = (lax.axis_size(a) for a in ALL)
    plane = ny * nx
    total_users = rows * plane * nz * nc
    cross = [(k, 1 - k) for k in range(nc)]

    cols = nx * nc
    fetch = [
        (((z + SHIFT[k]) % nz) * cols + k, z * cols + k) for z in range(nz) for k in range(cols)
    ]
    packed, count = call(
        pack_kernel,
        (bf16(plane, rows + 8, width), f32(8, LANES)),
        *(users, positives[None], cohorts[None]),
        limit=None,
    )
    near = exchange(packed, PLANE)
    item_block = lax.ppermute(bank, COLUMN, fetch)
    flip = lambda axis, by: [(k, k ^ by) for k in range(lax.axis_size(axis))]
    others = [lax.ppermute(count, "z", flip("z", by)) for by in (4, 6, 2)]
    count = count + others[0] + others[1] + others[2]
    count = count + lax.ppermute(count, "c", cross)
    other_count = lax.ppermute(count, "z", flip("z", 1))
    far = lax.ppermute(near, "c", cross)

    near_stats, near_coh = forward(near, item_block, rows)
    other_near = lax.ppermute(near_stats, "c", cross)
    far_stats, far_coh = forward(far, item_block, rows)
    other_far = lax.ppermute(far_stats, "c", cross)
    stats = call(
        join_kernel,
        f32(plane, 2 * plane + 8, LANES),
        *(near_stats, far_stats, other_near, other_far, count, other_count),
    )
    stats = exchange(stats, PLANE)

    far_part, bank_part, lse, weight, loss = call(
        functools.partial(backward_far_kernel, rows, total_users / NCOH),
        (
            bf16(plane, width, rows),
            f32(*bank.shape),
            f32(2 * plane, LANES),
            f32(NCOH, LANES),
            f32(8, LANES),
        ),
        *(far, item_block, stats, near_coh, far_coh),
    )
    far_part = lax.ppermute(far_part, "c", cross)
    kept, bank_part = call(
        functools.partial(backward_near_kernel, rows),
        (bf16(plane // STEP, bank.shape[0], STEP * rows), bf16(bank.shape[0] + 8, width)),
        *(near, item_block, lse, weight, bank_part, loss),
        scratch=[pltpu.VMEM(bank.shape, F32)],
    )
    bank_part = lax.ppermute(bank_part, COLUMN, [(b, a) for a, b in fetch])
    user_part = call(users_near_kernel, bf16(plane, width, rows), *(kept, item_block, far_part))
    user_part = exchange(user_part, PLANE)
    half = bank.shape[0] // nc
    height = half // nx
    theirs = lax.ppermute(bank_part[: half + 8], "c", cross)
    pieces = call(halve_kernel, (bf16(height + 8, width),) * nx, bank_part, theirs)
    arrived = [pieces[0]]
    for r in range(1, nx):
        arrived.append(lax.ppermute(pieces[r], "x", [(k, (k + r) % nx) for k in range(nx)]))
    user_grad, bank_grad, loss = call(
        functools.partial(finish_kernel, 1.0 / total_users),
        (f32(rows, width), f32(height, width), f32(1, LANES)),
        *(user_part, *arrived),
    )
    return loss[0, 0], user_grad, bank_grad


def solution(mesh):
    torus = Mesh(mesh.devices.reshape(4, 8, 4, 2), ALL)
    return jax.shard_map(
        step,
        mesh=torus,
        in_specs=(P(ALL, None), P(("y", "z"), None), P(ALL), P(ALL)),
        out_specs=(P(), P(ALL, None), P(ALL, None)),
        check_vma=False,
    )
```

```python
import functools

import jax
import jax.numpy as jnp
from jax import lax
from jax.experimental import pallas as pl
from jax.experimental.pallas import tpu as pltpu
from jax.sharding import Mesh
from jax.sharding import PartitionSpec as P


NCOH = 16
PLANE = ("x", "y")
COLUMN = ("z", "x", "c")
ALL = ("y", "z", "x", "c")
SHIFT = (0, 4, 1, 5, 7, 3, 2, 6)
F32 = jnp.float32
BF16 = jnp.bfloat16
LANES = 128
RADIX = 128
STEP = 4
VMEM = pl.BlockSpec(memory_space=pltpu.VMEM)


def call(kernel, out_shape, *operands, scratch=(), limit=24 << 20):
    return pl.pallas_call(
        kernel,
        in_specs=[VMEM] * len(operands),
        out_specs=jax.tree.map(lambda _: VMEM, out_shape),
        out_shape=out_shape,
        scratch_shapes=list(scratch),
        compiler_params=pltpu.CompilerParams(vmem_limit_bytes=limit),
    )(*operands)


def f32(*shape):
    return jax.ShapeDtypeStruct(shape, F32)


def bf16(*shape):
    return jax.ShapeDtypeStruct(shape, BF16)


def first_item(items):
    column = lax.axis_index("x") * lax.axis_size("c") + lax.axis_index("c")
    shift = sum(jnp.where(column == k, by, 0) for k, by in enumerate(SHIFT))
    nz = lax.axis_size("z")
    return (lax.axis_index("y") * nz + (lax.axis_index("z") + shift) % nz) * items


def exchange(value, axis):
    return lax.all_to_all(value, axis, split_axis=0, concat_axis=0, tiled=True)


def scores(bank, users):
    return lax.dot_general(bank, users, (((1,), (1,)), ((), ())), preferred_element_type=F32)


def iota(shape, dim):
    return lax.broadcasted_iota(jnp.int32, shape, dim)


def shard_users(packed, at, rows):
    return jnp.concatenate([packed[at + s, :rows, :] for s in range(STEP)], axis=0)


def shard_row(packed, at, row, half):
    cut = slice(half * LANES, (half + 1) * LANES)
    tiles = [packed[at + s, row : row + 8, cut].astype(F32)[0:1] for s in range(STEP)]
    return jnp.concatenate(tiles, axis=1)


def cohort_row(packed, at, rows, half):
    cut = slice(half * LANES, (half + 1) * LANES)
    tiles = [packed[at + s, rows : rows + 8, cut].astype(F32)[1:2] for s in range(STEP)]
    return jnp.concatenate(tiles, axis=1)


def local_positives(packed, at, rows, first):
    high = shard_row(packed, at, rows, 0)
    low = shard_row(packed, at, rows, 1)
    return (high * RADIX + low).astype(jnp.int32) - first


def column_to_row(column):
    shape = (NCOH, LANES)
    spread = jnp.where(iota(shape, 0) == iota(shape, 1), column, F32(0))
    return jnp.sum(spread, axis=0, keepdims=True)


def row_to_column(row):
    shape = (NCOH, LANES)
    spread = jnp.where(iota(shape, 0) == iota(shape, 1), row, F32(0))
    return jnp.sum(spread, axis=1, keepdims=True)


def pack_kernel(users, positives, cohorts, out, count):
    rows, _ = users.shape
    pos = positives[...]
    high = (pos // RADIX).astype(F32)
    low = (pos % RADIX).astype(F32)
    mine = cohorts[...].astype(F32)
    row = iota((8, LANES), 0)
    left = jnp.where(row == 0, high, jnp.where(row == 1, mine, F32(0))).astype(BF16)
    right = jnp.where(row == 0, low, F32(0)).astype(BF16)
    for k in range(out.shape[0]):
        out[k, :rows, :] = users[...]
        out[k, rows:, :LANES] = left
        out[k, rows:, LANES:] = right
    ids = iota((NCOH, LANES), 0).astype(F32)
    column = jnp.sum(jnp.where(ids == mine, F32(1), F32(0)), axis=1, keepdims=True)
    count[...] = jnp.broadcast_to(column_to_row(column), (8, LANES))


def forward_kernel(rows, packed, bank, stats, coh):
    shards = packed.shape[0]
    first = first_item(bank.shape[0])
    positive = jnp.zeros((NCOH, 1), F32)
    for at in range(0, shards, STEP):
        logits = scores(bank[...], shard_users(packed, at, rows))
        top = jnp.max(logits, axis=0, keepdims=True)
        total = jnp.sum(jnp.exp(logits - top), axis=0, keepdims=True)
        pos = local_positives(packed, at, rows, first)
        own = jnp.sum(jnp.where(iota(logits.shape, 0) == pos, logits, F32(0)), axis=0, keepdims=True)
        lse = top + jnp.log(total)
        mine = cohort_row(packed, at, rows, 0)
        ids = iota((NCOH, mine.shape[1]), 0).astype(F32)
        positive += jnp.sum(jnp.where(ids == mine, own, F32(0)), axis=1, keepdims=True)
        for s in range(STEP):
            cut = slice(s * LANES, (s + 1) * LANES)
            stats[at + s : at + s + 1, :] = lse[:, cut]
            coh[at + s : at + s + 1, :] = mine[:, cut]
    stats[shards:, :] = jnp.broadcast_to(column_to_row(positive), (8, LANES))


def forward(packed, bank, rows):
    shards = packed.shape[0]
    shapes = (f32(shards + 8, LANES), f32(shards, LANES))
    return call(functools.partial(forward_kernel, rows), shapes, packed, bank)


def join_kernel(near, far, other_near, other_far, count, other_count, out):
    shards = near.shape[0] - 8

    def join(a, b):
        top = jnp.maximum(a, b)
        return top + jnp.log(jnp.exp(a - top) + jnp.exp(b - top))

    first = join(near[:shards], other_far[:shards])
    second = join(far[:shards], other_near[:shards])
    positive = near[shards:] + far[shards:] + other_near[shards:] + other_far[shards:]
    extra = jnp.where(iota(positive.shape, 0) == 0, positive, count[...] + other_count[...])
    for k in range(out.shape[0]):
        out[k, :shards] = first
        out[k, shards : 2 * shards] = second
        out[k, 2 * shards :] = extra


def settle(scale, stats, coh_near, coh_far, lse_out, weight_out, loss_out):
    shards = coh_near.shape[0]
    both = 2 * shards
    top = stats[0, :both]
    for k in range(1, stats.shape[0]):
        top = jnp.maximum(top, stats[k, :both])
    total = jnp.exp(stats[0, :both] - top)
    rest = stats[0, both:]
    for k in range(1, stats.shape[0]):
        total += jnp.exp(stats[k, :both] - top)
        rest += stats[k, both:]
    lse = top + jnp.log(total)
    lse_out[...] = lse
    counts = row_to_column(rest[1:2])
    per_cohort = jnp.where(counts > 0, scale / jnp.maximum(counts, F32(1)), F32(0))
    weight_out[...] = jnp.broadcast_to(per_cohort, weight_out.shape)
    weights = jnp.zeros((both, LANES), F32)
    cohorts = jnp.concatenate([coh_near[...], coh_far[...]], axis=0)
    for c in range(NCOH):
        weights = jnp.where(cohorts == F32(c), per_cohort[c : c + 1, :], weights)
    loss = jnp.sum(weights * lse, keepdims=True)
    loss -= jnp.sum(per_cohort * row_to_column(rest[0:1]), keepdims=True)
    loss_out[...] = jnp.broadcast_to(loss, loss_out.shape)


def dlogits_at(rows, half, at, packed, bank, lse, weight):
    shards = packed.shape[0]
    users = shard_users(packed, at, rows)
    logits = scores(bank[...], users)
    pos = local_positives(packed, at, rows, first_item(bank.shape[0]))
    mine = cohort_row(packed, at, rows, 0)
    ids = iota((NCOH, mine.shape[1]), 0).astype(F32)
    weights = jnp.sum(jnp.where(ids == mine, weight[:, 0:1], F32(0)), axis=0, keepdims=True)
    line = half * shards + at
    level = jnp.concatenate([lse[line + s : line + s + 1, :] for s in range(STEP)], axis=1)
    hot = jnp.where(iota(logits.shape, 0) == pos, F32(1), F32(0))
    return users, (weights * (jnp.exp(logits - level) - hot)).astype(BF16)


def backward_far_kernel(rows, scale, packed, bank, stats, coh_near, coh_far, *outs):
    user_part, bank_part, lse, weight, loss = outs
    settle(scale, stats, coh_near, coh_far, lse, weight, loss)
    bank_t = bank[...].T
    total = None
    for at in range(0, packed.shape[0], STEP):
        users, dlogits = dlogits_at(rows, 1, at, packed, bank, lse, weight)
        part = jnp.dot(bank_t, dlogits, preferred_element_type=F32).astype(BF16)
        for s in range(STEP):
            user_part[at + s] = part[:, s * LANES : (s + 1) * LANES]
        grad = jnp.dot(dlogits, users, preferred_element_type=F32)
        total = grad if total is None else total + grad
    bank_part[...] = total


def digits_of(value):
    high = value.astype(BF16)
    rest = value - high.astype(F32)
    mid = rest.astype(BF16)
    low = (rest - mid.astype(F32)).astype(BF16)
    row = iota(value.shape, 0)
    zero = F32(0)
    tile = jnp.where(row == 0, high.astype(F32), zero)
    tile = jnp.where(row == 1, mid.astype(F32), tile)
    return jnp.where(row == 2, low.astype(F32), tile).astype(BF16)


def read_digits(tile):
    return jnp.sum(tile.astype(F32), axis=0, keepdims=True)[:, :LANES]


def write_digits(out, at, value):
    tile = digits_of(jnp.broadcast_to(value, (8, LANES)))
    out[at : at + 8, :LANES] = tile
    out[at : at + 8, LANES:] = tile


def backward_near_kernel(rows, packed, bank, lse, weight, far_part, loss, kept, out, acc):
    total = far_part[...]
    for step in range(packed.shape[0] // STEP):
        users, dlogits = dlogits_at(rows, 0, step * STEP, packed, bank, lse, weight)
        kept[step] = dlogits
        total = total + jnp.dot(dlogits, users, preferred_element_type=F32)
    acc[...] = total
    nx, nc = lax.axis_size("x"), lax.axis_size("c")
    height = acc.shape[0] // (nx * nc)
    core = lax.axis_index("c")
    for side, owner in enumerate((1 - core, core)):
        for r in range(nx):
            piece = (lax.axis_index("x") + r) % nx * nc + owner
            at = pl.multiple_of(piece * height, height)
            to = side * (nx * height + 8) + r * height
            out[to : to + height, :] = acc[pl.ds(at, height), :].astype(BF16)
    write_digits(out, nx * height, loss[...])


def users_near_kernel(kept, bank, far_part, user_part, parts, sems):
    bank_t = bank[...].T
    copies_out = []
    for step in range(kept.shape[0]):
        part = jnp.dot(bank_t, kept[step], preferred_element_type=F32)
        for s in range(STEP):
            mine = part[:, s * LANES : (s + 1) * LANES]
            at = step * STEP + s
            parts[at] = (mine + far_part[at].astype(F32)).astype(BF16)
        cut = pl.ds(step * STEP, STEP)
        copies_out.append(pltpu.make_async_copy(parts.at[cut], user_part.at[cut], sems.at[step]))
        copies_out[-1].start()
    for copy in copies_out:
        copy.wait()


def users_near(kept, bank, far_part):
    shape = bf16(*far_part.shape)
    steps = kept.shape[0]
    return pl.pallas_call(
        users_near_kernel,
        in_specs=[VMEM] * 3,
        out_specs=pl.BlockSpec(memory_space=pltpu.HBM),
        out_shape=shape,
        scratch_shapes=[pltpu.VMEM(shape.shape, BF16), pltpu.SemaphoreType.DMA((steps,))],
        compiler_params=pltpu.CompilerParams(vmem_limit_bytes=24 << 20),
        name="users_near",
    )(kept, bank, far_part)


def halve_kernel(mine, theirs, *pieces):
    below = theirs.shape[0]
    height = (below - 8) // len(pieces)
    loss = read_digits(mine[below - 8 : below, :]) + read_digits(theirs[below - 8 :, :])
    for r, piece in enumerate(pieces):
        cut = slice(below + r * height, below + (r + 1) * height)
        own = mine[cut, :].astype(F32) + theirs[r * height : (r + 1) * height, :].astype(F32)
        piece[:height, :] = own.astype(BF16)
        write_digits(piece, height, loss)


def finish_kernel(share, parts, *refs):
    pieces, (user_grad, bank_grad, loss) = refs[:-3], refs[-3:]
    total = parts[0].astype(F32)
    for k in range(1, parts.shape[0]):
        total = total + parts[k].astype(F32)
    user_grad[...] = total.T
    height = bank_grad.shape[0]
    total = pieces[0][...].astype(F32)
    for piece in pieces[1:]:
        total = total + piece[...].astype(F32)
    bank_grad[...] = total[:height]
    loss[...] = jnp.sum(total[height:], axis=0, keepdims=True)[:, :LANES] * share


def step(users, bank, positives, cohorts):
    rows, width = users.shape
    ny, nz, nx, nc = (lax.axis_size(a) for a in ALL)
    plane = ny * nx
    total_users = rows * plane * nz * nc
    cross = [(k, 1 - k) for k in range(nc)]

    cols = nx * nc
    fetch = [
        (((z + SHIFT[k]) % nz) * cols + k, z * cols + k) for z in range(nz) for k in range(cols)
    ]
    packed, count = call(
        pack_kernel,
        (bf16(plane, rows + 8, width), f32(8, LANES)),
        *(users, positives[None], cohorts[None]),
        limit=None,
    )
    near = exchange(packed, PLANE)
    item_block = lax.ppermute(bank, COLUMN, fetch)
    for axis, by in (("z", 4), ("z", 2), ("c", 1), ("z", 1)):
        ways = [(k, k ^ by) for k in range(lax.axis_size(axis))]
        other_count = lax.ppermute(count, axis, ways)
        if (axis, by) != ("z", 1):
            count = count + other_count
    far = lax.ppermute(near, "c", cross)

    near_stats, near_coh = forward(near, item_block, rows)
    other_near = lax.ppermute(near_stats, "c", cross)
    far_stats, far_coh = forward(far, item_block, rows)
    other_far = lax.ppermute(far_stats, "c", cross)
    stats = call(
        join_kernel,
        f32(plane, 2 * plane + 8, LANES),
        *(near_stats, far_stats, other_near, other_far, count, other_count),
    )
    stats = exchange(stats, PLANE)

    far_part, bank_part, lse, weight, loss = call(
        functools.partial(backward_far_kernel, rows, total_users / NCOH),
        (
            bf16(plane, width, rows),
            f32(*bank.shape),
            f32(2 * plane, LANES),
            f32(NCOH, LANES),
            f32(8, LANES),
        ),
        *(far, item_block, stats, near_coh, far_coh),
    )
    far_part = lax.ppermute(far_part, "c", cross)
    kept, bank_part = call(
        functools.partial(backward_near_kernel, rows),
        (bf16(plane // STEP, bank.shape[0], STEP * rows), bf16(bank.shape[0] + 8, width)),
        *(near, item_block, lse, weight, bank_part, loss),
        scratch=[pltpu.VMEM(bank.shape, F32)],
    )
    bank_part = lax.ppermute(bank_part, COLUMN, [(b, a) for a, b in fetch])
    user_part = users_near(kept, item_block, far_part)
    user_part = exchange(user_part, PLANE)
    half = bank.shape[0] // nc
    height = half // nx
    theirs = lax.ppermute(bank_part[: half + 8], "c", cross)
    pieces = call(halve_kernel, (bf16(height + 8, width),) * nx, bank_part, theirs)
    arrived = [pieces[0]]
    for r in range(1, nx):
        arrived.append(lax.ppermute(pieces[r], "x", [(k, (k + r) % nx) for k in range(nx)]))
    user_grad, bank_grad, loss = call(
        functools.partial(finish_kernel, 1.0 / total_users),
        (f32(rows, width), f32(height, width), f32(1, LANES)),
        *(user_part, *arrived),
    )
    return loss[0, 0], user_grad, bank_grad


def solution(mesh):
    torus = Mesh(mesh.devices.reshape(4, 8, 4, 2), ALL)
    return jax.shard_map(
        step,
        mesh=torus,
        in_specs=(P(ALL, None), P(("y", "z"), None), P(ALL), P(ALL)),
        out_specs=(P(), P(ALL, None), P(ALL, None)),
        check_vma=False,
    )
```
